32 devices in a mesh: seq: 2 (over core), batch: 16 (over z, y, x).
Axes of the slice: x: 2, y: 2, z: 4, core: 2. Of those that a mesh axis runs over, the one named last changes fastest.
Arguments:
- queries: bfloat16 [16, 1024, 1024], P('batch', 'seq'), may hold values from -6 to 6
- keys: bfloat16 [16, 1024, 1024], P('batch', 'seq'), may hold values from -6 to 6
- values: bfloat16 [16, 1024, 2048], P('batch', 'seq'), may hold values from -6 to 6
- gate_rate: bfloat16 [16, 1024, 1024], P('batch', 'seq'), may hold values from 0.5 to 2
- segment_ids: int32 [16, 1024], P('batch', 'seq'), may hold values from 0 to 2, never falling along the last dimension, each value on 1 to 512 neighbouring positions
- decay_exps: int32 [4], replicated, may hold values from 0 to 13
- out_weight: bfloat16 [2048, 2048], P('batch'), may hold values from -0.125 to 0.125
Outputs:
- projected: bfloat16 [16, 1024, 2048], P('batch', 'seq')
The draws below stay inside these ranges and needn't reach their ends.
Inputs may be any that keep to these rules, and one draw needn't show every extreme that they name: `segment_ids`: within each stream the ids never fall and start at 0; each of the 3 ids covers 1 to 512 consecutive tokens, one of them exactly 512.
All inputs are finite; a program needn't handle non-finite values.
Results may differ from the reference program's by a relative error of at most 0.004.
The reference program's roundings to bfloat16 on the way (of `hidden`) count: a program that leaves them out, or rounds other values in their place, can miss the bound.
Values may be sent and summed in bfloat16 or wider, within the bound.
A program may use at most 128 MiB of HBM per device.

```python
import math
import jax
import jax.numpy as jnp
import numpy as np
from jax import lax

D = 2048
HEADS = 4
HEAD_K = 256
BLOCK = 64
SEGS = 3
SEQLEN = 1024
GROUPS = 16
KEYS = 1024
VALS = 2048


def place_ends(values, own_key, low, top_value):
    longest = values.shape.index(max(values.shape))
    spots = []
    for shift in (0, 1):
        where = [jax.random.randint(jax.random.fold_in(own_key, axis), (), 0, length) for axis, length in enumerate(values.shape)]
        where[longest] = (where[longest] + shift) % values.shape[longest]
        spots.append(tuple(where))
    return values.at[spots[0]].set(low).at[spots[1]].set(top_value)


def steps_of(rng, extent, cuts, low, top_value):
    def one(position, blocks):
        draws = jax.random.uniform(jax.random.fold_in(jax.random.fold_in(rng, 6), position), (blocks,), jnp.float32, low / len(cuts), top_value / len(cuts))
        return jnp.repeat(jnp.exp(draws), extent[position] // blocks).reshape((-1,) + (1,) * (len(extent) - position - 1))

    level = one(*cuts[0])
    for cut in cuts[1:]:
        level = level * one(*cut)
    return level


def profile(count, total, reach, skew):
    portions = [(1 << 20) // math.isqrt(standing ** skew) + 1 for standing in range(2, count + 1)]
    surplus, holding = total - reach - (count - 1), [1] * (count - 1)
    while surplus > 0:
        movable = [i for i in range(count - 1) if holding[i] < reach]
        pool, remaining = sum([portions[i] for i in movable]), surplus
        for i in movable:
            extra = min(reach - holding[i], max(1, remaining * portions[i] // pool), surplus)
            holding[i] = holding[i] + extra
            surplus = surplus - extra
    return np.array([reach] + holding)


def ragged(own_key, number_of, total, most, skew):
    if number_of == 2:
        one = jax.random.randint(own_key, (), max(1, total - most), min(most, total - 1) + 1)
        return jnp.stack([one, total - one])
    sizes = jnp.asarray(profile(number_of, total, most, skew), jnp.int32)
    pairs = (number_of - 1) // 2
    giver, taker = sizes[1:1 + 2 * pairs:2], sizes[2:2 + 2 * pairs:2]
    margin = jnp.minimum(giver - 1, most - taker)
    shifted = jax.random.randint(jax.random.fold_in(own_key, 1), (pairs,), 0, 1 << 20) % (margin + 1)
    sizes = sizes.at[1:1 + 2 * pairs:2].set(giver - shifted).at[2:2 + 2 * pairs:2].set(taker + shifted)
    return sizes[jax.random.permutation(jax.random.fold_in(own_key, 2), number_of)]


def centred(stream_key, shape, scale, limit, cuts=(), kind=jnp.bfloat16):
    values = jax.random.normal(stream_key, shape, jnp.float32) * scale
    if len(cuts) > 0:
        values = steps_of(stream_key, shape, cuts, -0.22, 0.18) * values
    return jnp.clip(values, min=-limit, max=limit).astype(kind)


def setup_inputs(seed: int = 0) -> dict:
    arg_keys = jax.random.split(jax.random.key(seed), 8)
    return {
        "queries": centred(arg_keys[0], (GROUPS, SEQLEN, KEYS), 1.0, 6.0, ((0, 16), (1, 2))),
        "keys": centred(arg_keys[1], (GROUPS, SEQLEN, KEYS), 1.0, 6.0, ((0, 16), (1, 2))),
        "values": centred(arg_keys[2], (GROUPS, SEQLEN, VALS), 1.0, 6.0, ((0, 16), (1, 2))),
        "gate_rate": jnp.clip(jnp.exp(math.log(2.0) - 1.3862944 * jax.random.uniform(arg_keys[3], (GROUPS, SEQLEN, KEYS), jnp.float32) ** steps_of(arg_keys[3], (GROUPS, SEQLEN, KEYS), ((0, 16), (1, 2)), -0.2, 0.2)), 0.5, 2.0).astype(jnp.bfloat16),
        "segment_ids": jax.vmap(lambda own: jnp.searchsorted(jnp.cumsum(ragged(own, SEGS, SEQLEN, SEQLEN // 2, 2)), jnp.arange(SEQLEN), side="right"))(jax.random.split(arg_keys[4], GROUPS)).reshape((GROUPS, SEQLEN)).astype(jnp.int32),
        "decay_exps": place_ends(jax.random.randint(arg_keys[5], (HEADS,), 0, 14), jax.random.fold_in(arg_keys[5], 1), 0, 13).astype(jnp.int32),
        "out_weight": centred(arg_keys[6], (VALS, D), VALS ** -0.5, 0.125, ((0, 16),)),
    }


def linear_blocks(lifted_query, key_heads, value_heads, log_decay, starts, initial):
    groups, length, head_count, key_width = lifted_query.shape
    value_width = value_heads.shape[3]
    block_count = length // BLOCK

    def split(member):
        return jnp.swapaxes(member.reshape((groups, block_count, BLOCK) + member.shape[2:]), 0, 1)

    def advance(carried, pieces):
        query_rows, key_rows, value_rows, log_rows, start_rows = pieces
        running = jnp.cumsum(log_rows, axis=1)
        segment_rank = jnp.cumsum(start_rows, axis=1)
        unbroken = (segment_rank == 0).astype(jnp.float32)
        raised_q = query_rows * jnp.exp(running)
        raised_k = key_rows * jnp.exp(-running)
        scores = jnp.einsum('gthc,gshc->ghts', raised_q, raised_k, precision=lax.Precision.HIGHEST)
        order = jnp.arange(BLOCK)
        causal = order[:, None] >= order[None, :]
        same_doc = segment_rank[:, :, None] == segment_rank[:, None, :]
        allowed = jnp.logical_and(causal[None], same_doc).astype(jnp.float32)
        inside = jnp.einsum('ghts,gshv->gthv', scores * allowed[:, None], value_rows, precision=lax.Precision.HIGHEST)
        outside = unbroken[:, :, None, None] * jnp.einsum('gthc,ghcv->gthv', raised_q, carried, precision=lax.Precision.HIGHEST)
        final_log = running[:, -1]
        in_last = (segment_rank == segment_rank[:, -1:]).astype(jnp.float32)
        weighted = key_rows * jnp.exp(final_log[:, None] - running) * in_last[:, :, None, None]
        kept = unbroken[:, -1][:, None, None, None] * jnp.exp(final_log)[..., None] * carried
        updated = kept + jnp.einsum('gshc,gshv->ghcv', weighted, value_rows, precision=lax.Precision.HIGHEST)
        return (updated, inside + outside)
    members = (lifted_query, key_heads, value_heads, log_decay, starts)
    final, outputs = lax.scan(advance, initial, tuple((split(member) for member in members)))
    outputs = jnp.swapaxes(outputs, 0, 1).reshape(groups, length, head_count, value_width)
    return (outputs, final)

def reference(queries, keys, values, gate_rate, segment_ids, decay_exps, out_weight):
    groups = queries.shape[0]
    length = queries.shape[1]
    head_count = decay_exps.shape[0]

    def heads_of(array):
        return array.astype(jnp.float32).reshape(groups, length, head_count, -1)
    scaling = jnp.exp2(-decay_exps.astype(jnp.float32)) / 16.0
    log_decay = -heads_of(gate_rate) * scaling[None, None, :, None]
    previous = jnp.concatenate([jnp.full((groups, 1), -1, jnp.int32), segment_ids[:, :-1]], axis=1)
    starts = (segment_ids != previous).astype(jnp.float32)
    query_heads = heads_of(queries) * (1.0 / math.sqrt(HEAD_K))
    key_heads = heads_of(keys)
    value_heads = heads_of(values)
    initial = jnp.zeros((groups, head_count, key_heads.shape[3], value_heads.shape[3]), jnp.float32)
    mixed, final = linear_blocks(query_heads, key_heads, value_heads, log_decay, starts, initial)
    normed = mixed / jnp.sqrt(lax.optimization_barrier(jnp.mean(mixed * mixed, axis=-1, keepdims=True)) + 1.0)
    hidden = normed.astype(jnp.bfloat16).reshape(groups * length, -1)
    product = jnp.dot(hidden, out_weight, preferred_element_type=jnp.float32)
    return product.astype(jnp.bfloat16).reshape(groups, length, -1)
```

```python
import functools
import math

import jax
import jax.numpy as jnp
from jax import lax
from jax.experimental import pallas as pl
from jax.experimental.pallas import tpu as pltpu
from jax.sharding import PartitionSpec as P

MESH = pl.DeviceIdType.MESH
CHUNK = 256
TILE = 512
PIECES = 4


def chip_grid(mesh):
    count = mesh.shape["batch"]
    try:
        axis = mesh.axis_names.index("batch")
        line = mesh.devices.swapaxes(0, axis).reshape(count, -1)[:, 0]
        coords = [tuple(device.coords) for device in line]
        sizes = [len({c[i] for c in coords}) for i in (2, 1, 0)]
        lows = [min(c[i] for c in coords) for i in (2, 1, 0)]
        for index, c in enumerate(coords):
            z, y, x = (c[2] - lows[0], c[1] - lows[1], c[0] - lows[2])
            if (z * sizes[1] + y) * sizes[2] + x != index:
                return (count, 1, 1)
        return tuple(sizes)
    except Exception:
        return (count, 1, 1)


def split(x):
    high = x.astype(jnp.bfloat16)
    return high, (x - high.astype(jnp.float32)).astype(jnp.bfloat16)


def mm(a, b):
    return lax.dot_general(a, b, (((1,), (0,)), ((), ())), preferred_element_type=jnp.float32)


def mm_t(a, b):
    return lax.dot_general(a, b, (((1,), (1,)), ((), ())), preferred_element_type=jnp.float32)


def t_mm(a, b):
    return lax.dot_general(a, b, (((0,), (0,)), ((), ())), preferred_element_type=jnp.float32)


def thresholds(grid):
    Z, Y, X = grid
    beside, corner = X + Y - 2, (X - 1) * (Y - 1)
    picked = []
    for a in range(Z):
        best = None
        for reach in range(Z):
            far = [g for g in range(Z) if abs(g - a) > reach]
            below = a + corner * len([g for g in far if g < a])
            above = Z - 1 - a + corner * len([g for g in far if g > a])
            inside = (Z * beside + (Z - len(far)) * corner) / 2
            load = max(below, above, inside)
            if best is None or load < best[0]:
                best = (load, reach)
        picked.append(best[1])
    return picked


def kernel(
    grid, peers, heads, chunk, pieces,
    q_hbm, k_hbm, v_hbm, g_hbm, seg_ref, exps_ref, w_hbm,
    out_ref,
    q_ref, k_ref, v_ref, g_ref, w_ref, hidden, acc, seg_in, state_in, state_out,
    load_sem, seg_sem, state_send, state_recv, side_sem, relay_sem, climb_sem, corner_sem, recv_sem, msend, mrecv,
):
    Z, Y, X = grid
    s = lax.axis_index("seq")
    me = lax.axis_index("batch")
    length, keys = q_ref.shape
    key_width = keys // heads
    value_width = v_ref.shape[1] // heads
    rows = w_hbm.shape[0]
    depth = rows // pieces
    columns = w_ref.shape[1]
    part = columns // peers
    plane_rows = rows * X * Y
    a = me // (X * Y)
    swap = X == Y
    nb, nc = X, Y
    sides = [(db, 0) for db in range(1, nb)]
    fronts = [(0, dc) for dc in range(1, nc)]
    corners = [(db, dc) for db in range(1, nb) for dc in range(1, nc)]
    table = thresholds(grid)

    def strides(core):
        if not swap:
            return 1, X
        even = lax.rem(core, 2) == 0
        return jnp.where(even, 1, X), jnp.where(even, X, 1)

    def chip_at(core, plane, db, dc):
        sb, sc = strides(core)
        b = lax.rem(me // sb, nb)
        c = lax.rem(me // sc, nc)
        return (
            plane * (X * Y)
            + lax.rem(b - db + nb, nb) * sb
            + lax.rem(c - dc + nc, nc) * sc
        )

    near = jnp.minimum(a, Z - 1 - a)

    def plane_at(g):
        side = jnp.where(lax.rem(g, 2) == 1, -1, 1)
        rest = jnp.where(a < Z - 1 - a, g, Z - 1 - g)
        return jnp.where(g <= 2 * near, a + (g + 1) // 2 * side, rest)

    def reach_of(plane):
        reach = jnp.int32(table[0])
        for index in range(1, Z):
            reach = jnp.where(plane == index, table[index], reach)
        return reach

    reach = reach_of(a)
    reach_by = {-1: reach_of(a - 1), 1: reach_of(a + 1)}
    has = {-1: a > 0, 1: a < Z - 1}

    def label(plane, db, dc):
        return (plane * nb + db) * nc + dc

    def block(core, start, count):
        return w_ref.at[
            pl.ds(pl.multiple_of(start, depth), count),
            pl.ds(pl.multiple_of(core * part, part), part),
        ]

    def send(held, to, sem, device, piece):
        here = block(s, chip_at(s, *held) * rows + piece * depth, depth)
        return pltpu.make_async_remote_copy(
            src_ref=here, dst_ref=here, send_sem=sem, recv_sem=recv_sem.at[label(*to) * pieces + piece],
            device_id={"batch": device}, device_id_type=MESH,
        )

    def sideways(plane, piece):
        for db, _ in sides:
            send((plane, 0, 0), (plane, db, 0), side_sem.at[0], chip_at(s, a, -db, 0), piece).start()

    def forwards(plane, piece):
        for _, dc in fronts:
            send((plane, 0, 0), (plane, 0, dc), side_sem.at[1], chip_at(s, a, 0, -dc), piece).start()

    def climb(plane, side, piece):
        to = (plane, 0, 0)
        send(to, to, climb_sem.at[(side + 1) // 2, plane], me + side * X * Y, piece).start()

    def climb_corners(plane, side, piece):
        for corner in corners:
            to = (plane, *corner)
            send(to, to, corner_sem.at[(side + 1) // 2, plane], me + side * X * Y, piece).start()

    def wait_piece(plane, db, dc, piece):
        to = (plane, db, dc)
        send(to, to, side_sem.at[0], lax.rem(me + 1, X * Y * Z), piece).wait_recv()

    def share(plane, db, dc, piece):
        here = block(s, chip_at(s, plane, db, dc) * rows + piece * depth, depth)
        for ds in range(1, peers):
            pltpu.make_async_remote_copy(
                src_ref=here, dst_ref=here,
                send_sem=msend.at[ds - 1], recv_sem=mrecv.at[ds - 1, plane],
                device_id={"seq": lax.rem(s + ds, peers)}, device_id_type=MESH,
            ).start()

    def bulk(count, send_end, recv_end, core=0):
        here = block(core, 0, count * rows)
        return pltpu.make_async_remote_copy(
            src_ref=here, dst_ref=here, send_sem=send_end, recv_sem=recv_end,
            device_id={"batch": lax.rem(me + 1, X * Y * Z)}, device_id_type=MESH,
        )

    def inside(plane):
        return jnp.logical_and(plane >= 0, plane < Z)

    def needs(distance, side):
        return jnp.logical_and(has[side], distance + 1 > reach_by[side])

    def stage(d, piece):
        e = d - 2
        for side in (-1, 1):
            plane = a + side * d

            @pl.when(inside(plane))
            def _():
                wait_piece(plane, 0, 0, piece)
                pl.when(has[-side])(lambda: climb(plane, -side, piece))
                sideways(plane, piece)
                share(plane, 0, 0, piece)

            beside = a + side * (d - 1)
            on = jnp.logical_and(inside(beside), d - 1 <= reach)
            if side == 1:
                on = jnp.logical_and(on, d > 1)

            @pl.when(on)
            def _():
                for db, _ in sides:
                    wait_piece(beside, db, 0, piece)
                    for _, dc in fronts:
                        send(
                            (beside, db, 0), (beside, db, dc), relay_sem.at[beside],
                            chip_at(s, a, 0, -dc), piece,
                        ).start()
                    share(beside, db, 0, piece)

            if corners:
                far = a + side * e
                on = jnp.logical_or(e > reach, needs(e, -side))
                if side == 1:
                    on = jnp.logical_and(on, e > 0)
                else:
                    on = jnp.logical_or(on, e == 0)
                on = jnp.logical_and(on, jnp.logical_and(inside(far), e >= 0))

                @pl.when(on)
                def _():
                    for corner in corners:
                        wait_piece(far, *corner, piece)
                    pl.when(needs(e, -side))(lambda: climb_corners(far, -side, piece))
                    if side == -1:
                        pl.when(jnp.logical_and(e == 0, needs(e, side)))(lambda: climb_corners(far, side, piece))
                    for corner in corners:
                        share(far, *corner, piece)

    def stage_all(d, lo=0, hi=pieces):
        def one(piece, _):
            stage(d, piece)
            return 0

        lax.fori_loop(lo, hi, one, 0)

    def front_all(d):
        def one(piece, _):
            for side in (-1, 1):
                plane = a + side * d
                pl.when(inside(plane))(lambda: forwards(plane, piece))
            return 0

        lax.fori_loop(0, pieces, one, 0)

    def finish(g, lo=0, hi=pieces):
        plane = plane_at(g)
        distance = jnp.abs(plane - a)
        side = jnp.where(plane < a, -1, 1)
        onward = jnp.where(side < 0, needs(distance, 1), needs(distance, -1))

        def one(piece, _):
            @pl.when(distance > reach)
            def _():
                for db, _ in sides:
                    wait_piece(plane, db, 0, piece)
                    share(plane, db, 0, piece)

            for _, dc in fronts:
                wait_piece(plane, 0, dc, piece)
                share(plane, 0, dc, piece)

            if corners:
                late = jnp.logical_and(distance <= reach, jnp.logical_not(onward))

                @pl.when(jnp.logical_and(late, distance > 0))
                def _():
                    for corner in corners:
                        wait_piece(plane, *corner, piece)
                        share(plane, *corner, piece)
            return 0

        lax.fori_loop(lo, hi, one, 0)

    def mirrored(g):
        plane = plane_at(g)
        for ds in range(1, peers):
            core = lax.rem(s - ds + peers, peers)

            def wait(count):
                if count:
                    bulk(count, msend.at[ds - 1], mrecv.at[ds - 1, plane], core).wait_recv()

            if isinstance(g, int):
                wait(X * Y - 1 if g == 0 else X * Y)
            else:
                wait(X * Y)

    loads = [
        pltpu.make_async_copy(
            w_hbm, w_ref.at[pl.ds(pl.multiple_of(me * rows, rows), rows), :], load_sem.at[0]
        ),
        pltpu.make_async_copy(g_hbm, g_ref, load_sem.at[1]),
        pltpu.make_async_copy(k_hbm, k_ref, load_sem.at[2]),
        pltpu.make_async_copy(q_hbm, q_ref, load_sem.at[3]),
        pltpu.make_async_copy(v_hbm, v_ref, load_sem.at[4]),
    ]
    for load in loads:
        load.start()

    barrier = pltpu.get_barrier_semaphore()
    friends = [{"batch": chip_at(s, a, d, 0)} for d in range(1, nb)]
    friends += [{"batch": chip_at(s, a, 0, d)} for d in range(1, nc)]
    friends += [{"seq": lax.rem(s + d, peers)} for d in range(1, peers)]
    for friend in friends:
        pl.semaphore_signal(barrier, inc=1, device_id=friend, device_id_type=MESH)

    @pl.when(a < Z - 1)
    def _():
        pl.semaphore_signal(barrier, inc=1, device_id={"batch": me + X * Y}, device_id_type=MESH)

    @pl.when(a > 0)
    def _():
        pl.semaphore_signal(barrier, inc=1, device_id={"batch": me - X * Y}, device_id_type=MESH)

    above, below = jnp.where(a < Z - 1, 1, 0), jnp.where(a > 0, 1, 0)
    pl.semaphore_wait(barrier, len(friends) + above + below)

    loads[0].wait()

    def own(piece, _):
        for side in (-1, 1):
            pl.when(has[side])(lambda: climb(a, side, piece))
        sideways(a, piece)
        forwards(a, piece)
        return 0

    lax.fori_loop(0, pieces, own, 0)

    def next_core():
        return {"seq": lax.rem(s + 1, peers)}

    seg_copy = pltpu.make_async_remote_copy(
        src_ref=seg_ref, dst_ref=seg_in, send_sem=seg_sem.at[0], recv_sem=seg_sem.at[1],
        device_id=next_core(), device_id_type=MESH,
    )

    def state_copy(h):
        return pltpu.make_async_remote_copy(
            src_ref=state_out.at[h], dst_ref=state_in.at[h],
            send_sem=state_send.at[h], recv_sem=state_recv.at[h],
            device_id=next_core(), device_id_type=MESH,
        )

    @pl.when(s < peers - 1)
    def _():
        seg_copy.start()

    @pl.when(s == 0)
    def _():
        state_in[...] = jnp.zeros_like(state_in)
        seg_in[...] = jnp.full(seg_in.shape, -1, jnp.int32)

    for load in loads[1:]:
        load.wait()

    @pl.when(s > 0)
    def _():
        seg_copy.wait_recv()

    order_t = lax.broadcasted_iota(jnp.int32, (chunk, chunk), 0)
    order_s = lax.broadcasted_iota(jnp.int32, (chunk, chunk), 1)
    causal = order_t >= order_s
    triangle = jnp.where(causal, 1.0, 0.0).astype(jnp.bfloat16)
    seg_row = seg_ref[...].astype(jnp.float32)
    before = seg_in[...].astype(jnp.float32)[:, length - 1:]
    seg_wide = jnp.broadcast_to(seg_row, (128, length)).T

    def first():
        stage_all(1, 0, pieces // 2)

    def second():
        stage_all(1, pieces // 2, pieces)
        front_all(1)

    events = [first, second]
    turns = [1, 2]
    early = min(len(events), max(heads - 2, 0))

    def head(h, _):
        turn = h - jnp.where(s == 0, 1, 0)
        for number, event in zip(turns[:early], events):
            pl.when(turn == number)(event)

        exponent = jnp.full((1, key_width), exps_ref[h], jnp.int32).astype(jnp.float32)
        scale = jnp.exp2(-exponent) * (-1.0 / 16.0)

        @pl.when(s > 0)
        def _():
            state_copy(h).wait_recv()

        state = state_in[h]
        previous = before
        key_cols = pl.ds(pl.multiple_of(h * key_width, key_width), key_width)
        value_cols = pl.ds(pl.multiple_of(h * value_width, value_width), value_width)
        for i in range(length // chunk):
            now = pl.ds(i * chunk, chunk)
            log = mm(triangle, g_ref[now, key_cols]) * scale
            fall = jnp.exp(log)
            raised_q = q_ref[now, key_cols].astype(jnp.float32) * (fall * (1.0 / math.sqrt(key_width)))
            raised_k = k_ref[now, key_cols].astype(jnp.float32) * jnp.exp(-log)
            value = v_ref[now, value_cols]
            q_hi, q_lo = split(raised_q)
            k_hi, k_lo = split(raised_k)
            row = seg_row[:, i * chunk:(i + 1) * chunk]
            column = seg_wide[i * chunk:(i + 1) * chunk, :1]
            scores = mm_t(q_hi, k_hi) + mm_t(q_hi, k_lo) + mm_t(q_lo, k_hi)
            scores = jnp.where(jnp.logical_and(causal, column == row), scores, 0.0)
            p_hi, p_lo = split(scores)
            s_hi, s_lo = split(state)
            carried = mm_t(q_hi, s_hi) + mm_t(q_hi, s_lo) + mm_t(q_lo, s_hi)
            mixed = mm(p_hi, value) + mm(p_lo, value)
            mixed = mixed + jnp.where(column == previous, carried, 0.0)
            power = jnp.mean(mixed * mixed, axis=-1, keepdims=True)
            hidden[now, value_cols] = (mixed * lax.rsqrt(power + 1.0)).astype(jnp.bfloat16)
            final = fall[chunk - 1:, :]
            last = row[:, chunk - 1:]
            weighted = jnp.where(column == last, raised_k * final, 0.0)
            w_hi, w_lo = split(weighted)
            kept = jnp.where(last == previous, state * final, 0.0)
            state = kept + t_mm(value, w_hi) + t_mm(value, w_lo)
            previous = last

        @pl.when(s < peers - 1)
        def _():
            state_out[h] = state
            state_copy(h).start()

        return 0

    lax.fori_loop(0, heads, head, 0)
    for event in events[early:]:
        event()

    def plane_start(g):
        return pl.multiple_of(plane_at(g) * plane_rows, plane_rows)

    def project(g, first=False, last=False):
        start = plane_start(g)
        left = hidden[:, pl.ds(start, plane_rows)]
        for tile in range(columns // TILE):
            cols = pl.ds(tile * TILE, TILE)
            product = mm(left, w_ref[pl.ds(start, plane_rows), cols])
            if not first:
                product = acc[:, cols] + product
            if last:
                out_ref[:, cols] = product.astype(jnp.bfloat16)
            else:
                acc[:, cols] = product

    def ready(g):
        finish(g)
        mirrored(g)

    stage_all(2)
    front_all(2)
    if Z > 1:
        ready(0)
        project(0, first=True)

    def later(d, _):
        stage_all(d)
        front_all(d)
        return 0

    def middle(g, _):
        ready(g)
        project(g)
        return 0

    lax.fori_loop(3, Z + 1, later, 0)
    lax.fori_loop(1, Z - 2, middle, 0)
    half = pieces // 2
    if Z > 1:
        stage_all(Z + 1, 0, half)
        if Z > 2:
            ready(Z - 2)
            project(Z - 2)
        finish(Z - 1, 0, half)

        def closing(piece, _):
            stage(Z + 1, piece)
            finish(Z - 1, piece, piece + 1)
            return 0

        lax.fori_loop(half, pieces, closing, 0)
    else:
        finish(0)

    @pl.when(s < peers - 1)
    def _():
        seg_copy.wait_send()

        def sent(h, _):
            state_copy(h).wait_send()
            return 0

        lax.fori_loop(0, heads, sent, 0)

    if sides:
        bulk(Z * len(sides), side_sem.at[0], recv_sem.at[0]).wait_send()
    if fronts:
        bulk(Z * len(fronts), side_sem.at[1], recv_sem.at[0]).wait_send()

    def sent_plane(plane, _):
        if corners:
            @pl.when(jnp.abs(plane - a) <= reach)
            def _():
                bulk(len(corners), relay_sem.at[plane], recv_sem.at[0]).wait_send()

        for side in (-1, 1):
            away = (a - plane) * side
            on = jnp.logical_and(has[side], away >= 0)

            @pl.when(on)
            def _():
                bulk(1, climb_sem.at[(side + 1) // 2, plane], recv_sem.at[0]).wait_send()

            if corners:
                @pl.when(jnp.logical_and(on, away + 1 > reach_by[side]))
                def _():
                    bulk(len(corners), corner_sem.at[(side + 1) // 2, plane], recv_sem.at[0]).wait_send()

        return 0

    lax.fori_loop(0, Z, sent_plane, 0)
    mirrored(Z - 1)
    project(Z - 1, first=Z == 1, last=True)
    if X * Y * Z > 1:
        for ds in range(1, peers):
            bulk(X * Y * Z - 1, msend.at[ds - 1], recv_sem.at[0]).wait_send()


def local(grid, peers, queries, keys, values, gate_rate, segment_ids, decay_exps, out_weight):
    groups, length, key_features = queries.shape
    heads = decay_exps.shape[0]
    features = values.shape[2]
    columns = out_weight.shape[1]
    chips = grid[0] * grid[1] * grid[2]
    chunk = min(CHUNK, length)
    rows = out_weight.shape[0]
    pieces = PIECES if rows % (PIECES * 16) == 0 else 1
    kw, vw = key_features // heads, features // heads
    bf16, f32 = jnp.bfloat16, jnp.float32
    anywhere = pl.BlockSpec(memory_space=pl.ANY)
    call = pl.pallas_call(
        functools.partial(kernel, grid, peers, heads, chunk, pieces),
        out_shape=pltpu.VMEM((length, columns), bf16),
        in_specs=[anywhere] * 4
        + [pl.BlockSpec(memory_space=pltpu.VMEM), pl.BlockSpec(memory_space=pltpu.SMEM), anywhere],
        out_specs=pl.BlockSpec(memory_space=pltpu.VMEM),
        scratch_shapes=[
            pltpu.VMEM((length, key_features), bf16),
            pltpu.VMEM((length, key_features), bf16),
            pltpu.VMEM((length, features), bf16),
            pltpu.VMEM((length, key_features), bf16),
            pltpu.VMEM((features, columns), bf16),
            pltpu.VMEM((length, features), bf16),
            pltpu.VMEM((length, columns), f32),
            pltpu.VMEM((1, length), jnp.int32),
            pltpu.VMEM((heads, vw, kw), f32),
            pltpu.VMEM((heads, vw, kw), f32),
            pltpu.SemaphoreType.DMA((5,)),
            pltpu.SemaphoreType.DMA((2,)),
            pltpu.SemaphoreType.DMA((heads,)),
            pltpu.SemaphoreType.DMA((heads,)),
            pltpu.SemaphoreType.DMA((2,)),
            pltpu.SemaphoreType.DMA((grid[0],)),
            pltpu.SemaphoreType.DMA((2, grid[0])),
            pltpu.SemaphoreType.DMA((2, grid[0])),
            pltpu.SemaphoreType.DMA((chips * pieces,)),
            pltpu.SemaphoreType.DMA((max(peers - 1, 1),)),
            pltpu.SemaphoreType.DMA((max(peers - 1, 1), grid[0])),
        ],
        compiler_params=pltpu.CompilerParams(
            collective_id=0, has_side_effects=True, vmem_limit_bytes=61 * 1024 * 1024
        ),
        name="gla_project",
    )
    outs = [
        call(queries[n], keys[n], values[n], gate_rate[n], segment_ids[n:n + 1], decay_exps, out_weight)
        for n in range(groups)
    ]
    return jnp.stack(outs)


def solution(mesh):
    in_specs = (
        P("batch", "seq", None),
        P("batch", "seq", None),
        P("batch", "seq", None),
        P("batch", "seq", None),
        P("batch", "seq"),
        P(),
        P("batch", None),
    )
    body = functools.partial(local, chip_grid(mesh), mesh.shape["seq"])
    return jax.shard_map(
        body, mesh=mesh, in_specs=in_specs, out_specs=P("batch", "seq", None), check_vma=False
    )
```

```python
import functools
import math

import jax
import jax.numpy as jnp
from jax import lax
from jax.experimental import pallas as pl
from jax.experimental.pallas import tpu as pltpu
from jax.sharding import PartitionSpec as P

MESH = pl.DeviceIdType.MESH
CHUNK = 256
TILE = 512
PIECES = 4


def chip_grid(mesh):
    count = mesh.shape["batch"]
    try:
        axis = mesh.axis_names.index("batch")
        line = mesh.devices.swapaxes(0, axis).reshape(count, -1)[:, 0]
        coords = [tuple(device.coords) for device in line]
        sizes = [len({c[i] for c in coords}) for i in (2, 1, 0)]
        lows = [min(c[i] for c in coords) for i in (2, 1, 0)]
        for index, c in enumerate(coords):
            z, y, x = (c[2] - lows[0], c[1] - lows[1], c[0] - lows[2])
            if (z * sizes[1] + y) * sizes[2] + x != index:
                return (count, 1, 1)
        return tuple(sizes)
    except Exception:
        return (count, 1, 1)


def split(x):
    high = x.astype(jnp.bfloat16)
    return high, (x - high.astype(jnp.float32)).astype(jnp.bfloat16)


def mm(a, b):
    return lax.dot_general(a, b, (((1,), (0,)), ((), ())), preferred_element_type=jnp.float32)


def mm_t(a, b):
    return lax.dot_general(a, b, (((1,), (1,)), ((), ())), preferred_element_type=jnp.float32)


def t_mm(a, b):
    return lax.dot_general(a, b, (((0,), (0,)), ((), ())), preferred_element_type=jnp.float32)


def thresholds(grid):
    Z, Y, X = grid
    beside, corner = X + Y - 2, (X - 1) * (Y - 1)
    picked = []
    for a in range(Z):
        best = None
        for reach in range(Z):
            far = [g for g in range(Z) if abs(g - a) > reach]
            below = a + corner * len([g for g in far if g < a])
            above = Z - 1 - a + corner * len([g for g in far if g > a])
            inside = (Z * beside + (Z - len(far)) * corner) / 2
            load = max(below, above, inside)
            if best is None or load < best[0]:
                best = (load, reach)
        picked.append(best[1])
    return picked


def kernel(
    grid, peers, heads, chunk, pieces,
    q_hbm, k_hbm, v_hbm, g_hbm, seg_ref, exps_ref, w_hbm,
    out_ref,
    q_ref, k_ref, v_ref, g_ref, w_ref, hidden, acc, seg_in, state_in, state_out,
    load_sem, seg_sem, state_send, state_recv, side_sem, relay_sem, climb_sem, corner_sem, recv_sem, msend, mrecv,
):
    Z, Y, X = grid
    s = lax.axis_index("seq")
    me = lax.axis_index("batch")
    length, keys = q_ref.shape
    key_width = keys // heads
    value_width = v_ref.shape[1] // heads
    rows = w_hbm.shape[0]
    columns = w_ref.shape[1]
    part = columns // peers
    width = part // pieces
    plane_rows = rows * X * Y
    a = me // (X * Y)
    swap = X == Y
    nb, nc = X, Y
    sides = [(db, 0) for db in range(1, nb)]
    fronts = [(0, dc) for dc in range(1, nc)]
    corners = [(db, dc) for db in range(1, nb) for dc in range(1, nc)]
    table = thresholds(grid)

    def strides(core):
        if not swap:
            return 1, X
        even = lax.rem(core, 2) == 0
        return jnp.where(even, 1, X), jnp.where(even, X, 1)

    def chip_at(core, plane, db, dc):
        sb, sc = strides(core)
        b = lax.rem(me // sb, nb)
        c = lax.rem(me // sc, nc)
        return (
            plane * (X * Y)
            + lax.rem(b - db + nb, nb) * sb
            + lax.rem(c - dc + nc, nc) * sc
        )

    near = jnp.minimum(a, Z - 1 - a)

    def plane_at(g):
        side = jnp.where(lax.rem(g, 2) == 1, -1, 1)
        rest = jnp.where(a < Z - 1 - a, g, Z - 1 - g)
        return jnp.where(g <= 2 * near, a + (g + 1) // 2 * side, rest)

    def reach_of(plane):
        reach = jnp.int32(table[0])
        for index in range(1, Z):
            reach = jnp.where(plane == index, table[index], reach)
        return reach

    reach = reach_of(a)
    reach_by = {-1: reach_of(a - 1), 1: reach_of(a + 1)}
    has = {-1: a > 0, 1: a < Z - 1}

    def label(plane, db, dc):
        return (plane * nb + db) * nc + dc

    def block(core, start, count, piece, pieces_wide=1):
        return w_ref.at[
            pl.ds(pl.multiple_of(start, rows), count),
            pl.ds(pl.multiple_of(core * part + piece * width, width), pieces_wide * width),
        ]

    def send(held, to, sem, device, piece):
        here = block(s, chip_at(s, *held) * rows, rows, piece)
        return pltpu.make_async_remote_copy(
            src_ref=here, dst_ref=here, send_sem=sem, recv_sem=recv_sem.at[label(*to) * pieces + piece],
            device_id={"batch": device}, device_id_type=MESH,
        )

    def sideways(plane, piece):
        for db, _ in sides:
            send((plane, 0, 0), (plane, db, 0), side_sem.at[0], chip_at(s, a, -db, 0), piece).start()

    def forwards(plane, piece):
        for _, dc in fronts:
            send((plane, 0, 0), (plane, 0, dc), side_sem.at[1], chip_at(s, a, 0, -dc), piece).start()

    def climb(plane, side, piece):
        to = (plane, 0, 0)
        send(to, to, climb_sem.at[(side + 1) // 2, plane], me + side * X * Y, piece).start()

    def climb_corners(plane, side, piece):
        for corner in corners:
            to = (plane, *corner)
            send(to, to, corner_sem.at[(side + 1) // 2, plane], me + side * X * Y, piece).start()

    def wait_piece(plane, db, dc, piece):
        to = (plane, db, dc)
        send(to, to, side_sem.at[0], lax.rem(me + 1, X * Y * Z), piece).wait_recv()

    def share(plane, db, dc, piece):
        here = block(s, chip_at(s, plane, db, dc) * rows, rows, piece)
        for ds in range(1, peers):
            pltpu.make_async_remote_copy(
                src_ref=here, dst_ref=here,
                send_sem=msend.at[ds - 1], recv_sem=mrecv.at[ds - 1, plane * pieces + piece],
                device_id={"seq": lax.rem(s + ds, peers)}, device_id_type=MESH,
            ).start()

    def bulk(count, send_end, recv_end, core=0, piece=0, pieces_wide=pieces):
        here = block(core, 0, count * rows, piece, pieces_wide)
        return pltpu.make_async_remote_copy(
            src_ref=here, dst_ref=here, send_sem=send_end, recv_sem=recv_end,
            device_id={"batch": lax.rem(me + 1, X * Y * Z)}, device_id_type=MESH,
        )

    def inside(plane):
        return jnp.logical_and(plane >= 0, plane < Z)

    def needs(distance, side):
        return jnp.logical_and(has[side], distance + 1 > reach_by[side])

    def stage(d, piece):
        for side in (-1, 1):
            plane = a + side * d

            @pl.when(inside(plane))
            def _():
                wait_piece(plane, 0, 0, piece)
                pl.when(has[-side])(lambda: climb(plane, -side, piece))
                pl.when(d < Z - 1)(lambda: sideways(plane, piece))
                share(plane, 0, 0, piece)

        @pl.when(d == 1)
        def _():
            for db, _ in sides:
                wait_piece(a, db, 0, piece)
                for _, dc in fronts:
                    send((a, db, 0), (a, db, dc), relay_sem.at[a], chip_at(s, a, 0, -dc), piece).start()
                share(a, db, 0, piece)

        if not corners:
            return

        f = d - 2
        for side in (-1, 1):
            plane = a + side * f

            @pl.when(jnp.logical_and(jnp.logical_and(f > 0, f <= reach), inside(plane)))
            def _():
                for _, dc in fronts:
                    wait_piece(plane, 0, dc, piece)
                    for db, _ in sides:
                        send(
                            (plane, 0, dc), (plane, db, dc), relay_sem.at[plane],
                            chip_at(s, a, -db, 0), piece,
                        ).start()
                    share(plane, 0, dc, piece)

        def corner_step(plane, distance, side, both):
            for corner in corners:
                wait_piece(plane, *corner, piece)
            pl.when(needs(distance, -side))(lambda: climb_corners(plane, -side, piece))
            if both:
                pl.when(needs(distance, side))(lambda: climb_corners(plane, side, piece))
            for corner in corners:
                share(plane, *corner, piece)

        pl.when(d == 2)(lambda: corner_step(a, 0, -1, True))
        for side in (-1, 1):
            late = a + side * (d - 3)
            on = jnp.logical_and(jnp.logical_and(d > 3, d - 3 <= reach), needs(d - 3, -side))
            pl.when(jnp.logical_and(on, inside(late)))(lambda: corner_step(late, d - 3, side, False))
        for side in (-1, 1):
            far = a + side * f
            on = jnp.logical_and(jnp.logical_and(f > 0, f > reach), inside(far))
            pl.when(on)(lambda: corner_step(far, f, side, False))

    def stage_all(d, lo=0, hi=pieces):
        def one(piece, _):
            stage(d, piece)
            return 0

        lax.fori_loop(lo, hi, one, 0)

    def front_all(d):
        def one(piece, _):
            for side in (-1, 1):
                plane = a + side * d

                @pl.when(inside(plane))
                def _():
                    pl.when(d == Z - 1)(lambda: sideways(plane, piece))
                    forwards(plane, piece)
            return 0

        lax.fori_loop(0, pieces, one, 0)

    def finish(g, lo=0, hi=pieces, beside=True, rest=True, ahead=True):
        plane = plane_at(g)
        distance = jnp.abs(plane - a)
        side = jnp.where(plane < a, -1, 1)
        onward = jnp.where(side < 0, needs(distance, 1), needs(distance, -1))
        near_by = distance <= reach

        def one(piece, _):
            if beside:
                for db, _ in sides:
                    @pl.when(distance > 0)
                    def _():
                        wait_piece(plane, db, 0, piece)
                        share(plane, db, 0, piece)

            if ahead:
                for _, dc in fronts:
                    @pl.when(jnp.logical_or(distance == 0, jnp.logical_not(near_by)) if corners else distance >= 0)
                    def _():
                        wait_piece(plane, 0, dc, piece)
                        share(plane, 0, dc, piece)

            if corners and rest:
                late = jnp.logical_and(near_by, jnp.logical_not(onward))

                @pl.when(jnp.logical_and(late, distance > 0))
                def _():
                    for corner in corners:
                        wait_piece(plane, *corner, piece)
                        share(plane, *corner, piece)
            return 0

        lax.fori_loop(lo, hi, one, 0)

    def mirrored(g, piece):
        plane = plane_at(g)
        for ds in range(1, peers):
            core = lax.rem(s - ds + peers, peers)
            count = X * Y - 1 if isinstance(g, int) and g == 0 else X * Y
            if count:
                bulk(
                    count, msend.at[ds - 1], mrecv.at[ds - 1, plane * pieces + piece], core, piece, 1
                ).wait_recv()

    loads = [
        pltpu.make_async_copy(
            w_hbm, w_ref.at[pl.ds(pl.multiple_of(me * rows, rows), rows), :], load_sem.at[0]
        ),
        pltpu.make_async_copy(g_hbm, g_ref, load_sem.at[1]),
        pltpu.make_async_copy(k_hbm, k_ref, load_sem.at[2]),
        pltpu.make_async_copy(q_hbm, q_ref, load_sem.at[3]),
        pltpu.make_async_copy(v_hbm, v_ref, load_sem.at[4]),
    ]
    for load in loads:
        load.start()

    barrier = pltpu.get_barrier_semaphore()
    friends = [{"batch": chip_at(s, a, d, 0)} for d in range(1, nb)]
    friends += [{"batch": chip_at(s, a, 0, d)} for d in range(1, nc)]
    friends += [{"seq": lax.rem(s + d, peers)} for d in range(1, peers)]
    for friend in friends:
        pl.semaphore_signal(barrier, inc=1, device_id=friend, device_id_type=MESH)

    @pl.when(a < Z - 1)
    def _():
        pl.semaphore_signal(barrier, inc=1, device_id={"batch": me + X * Y}, device_id_type=MESH)

    @pl.when(a > 0)
    def _():
        pl.semaphore_signal(barrier, inc=1, device_id={"batch": me - X * Y}, device_id_type=MESH)

    above, below = jnp.where(a < Z - 1, 1, 0), jnp.where(a > 0, 1, 0)
    pl.semaphore_wait(barrier, len(friends) + above + below)

    loads[0].wait()

    def own(piece, _):
        for side in (-1, 1):
            pl.when(has[side])(lambda: climb(a, side, piece))
        sideways(a, piece)
        forwards(a, piece)
        return 0

    lax.fori_loop(0, pieces, own, 0)

    def next_core():
        return {"seq": lax.rem(s + 1, peers)}

    seg_copy = pltpu.make_async_remote_copy(
        src_ref=seg_ref, dst_ref=seg_in, send_sem=seg_sem.at[0], recv_sem=seg_sem.at[1],
        device_id=next_core(), device_id_type=MESH,
    )

    def state_copy(h):
        return pltpu.make_async_remote_copy(
            src_ref=state_out.at[h], dst_ref=state_in.at[h],
            send_sem=state_send.at[h], recv_sem=state_recv.at[h],
            device_id=next_core(), device_id_type=MESH,
        )

    @pl.when(s < peers - 1)
    def _():
        seg_copy.start()

    @pl.when(s == 0)
    def _():
        state_in[...] = jnp.zeros_like(state_in)
        seg_in[...] = jnp.full(seg_in.shape, -1, jnp.int32)

    for load in loads[1:]:
        load.wait()

    @pl.when(s > 0)
    def _():
        seg_copy.wait_recv()

    order_t = lax.broadcasted_iota(jnp.int32, (chunk, chunk), 0)
    order_s = lax.broadcasted_iota(jnp.int32, (chunk, chunk), 1)
    causal = order_t >= order_s
    triangle = jnp.where(causal, 1.0, 0.0).astype(jnp.bfloat16)
    seg_row = seg_ref[...].astype(jnp.float32)
    before = seg_in[...].astype(jnp.float32)[:, length - 1:]
    seg_wide = jnp.broadcast_to(seg_row, (128, length)).T

    quarter = pieces // 4

    def first():
        stage_all(1, 0, quarter)

    def second():
        stage_all(1, quarter, pieces - quarter)

    def third():
        stage_all(1, pieces - quarter, pieces)
        front_all(1)

    def fourth():
        stage_all(2, 0, pieces // 2)

    events = [first, second, third, fourth]
    lead = jnp.where(s == 0, 2, 0)

    def head(h, _):
        for number, event in enumerate(events):
            pl.when(h - lead == number)(event)

        exponent = jnp.full((1, key_width), exps_ref[h], jnp.int32).astype(jnp.float32)
        scale = jnp.exp2(-exponent) * (-1.0 / 16.0)

        @pl.when(s > 0)
        def _():
            state_copy(h).wait_recv()

        state = state_in[h]
        previous = before
        key_cols = pl.ds(pl.multiple_of(h * key_width, key_width), key_width)
        value_cols = pl.ds(pl.multiple_of(h * value_width, value_width), value_width)
        for i in range(length // chunk):
            now = pl.ds(i * chunk, chunk)
            log = mm(triangle, g_ref[now, key_cols]) * scale
            fall = jnp.exp(log)
            raised_q = q_ref[now, key_cols].astype(jnp.float32) * (fall * (1.0 / math.sqrt(key_width)))
            raised_k = k_ref[now, key_cols].astype(jnp.float32) * jnp.exp(-log)
            value = v_ref[now, value_cols]
            q_hi, q_lo = split(raised_q)
            k_hi, k_lo = split(raised_k)
            row = seg_row[:, i * chunk:(i + 1) * chunk]
            column = seg_wide[i * chunk:(i + 1) * chunk, :1]
            scores = mm_t(q_hi, k_hi) + mm_t(q_hi, k_lo) + mm_t(q_lo, k_hi)
            scores = jnp.where(jnp.logical_and(causal, column == row), scores, 0.0)
            p_hi, p_lo = split(scores)
            s_hi, s_lo = split(state)
            carried = mm_t(q_hi, s_hi) + mm_t(q_hi, s_lo) + mm_t(q_lo, s_hi)
            mixed = mm(p_hi, value) + mm(p_lo, value)
            mixed = mixed + jnp.where(column == previous, carried, 0.0)
            power = jnp.mean(mixed * mixed, axis=-1, keepdims=True)
            hidden[now, value_cols] = (mixed * lax.rsqrt(power + 1.0)).astype(jnp.bfloat16)
            final = fall[chunk - 1:, :]
            last = row[:, chunk - 1:]
            weighted = jnp.where(column == last, raised_k * final, 0.0)
            w_hi, w_lo = split(weighted)
            kept = jnp.where(last == previous, state * final, 0.0)
            state = kept + t_mm(value, w_hi) + t_mm(value, w_lo)
            previous = last

        @pl.when(s < peers - 1)
        def _():
            state_out[h] = state
            state_copy(h).start()

        return 0

    lax.fori_loop(0, heads, head, 0)
    for number, event in enumerate(events):
        pl.when(heads - lead <= number)(event)

    def plane_start(g):
        return pl.multiple_of(plane_at(g) * plane_rows, plane_rows)

    def project(g, first=False):
        start = plane_start(g)
        left = hidden[:, pl.ds(start, plane_rows)]
        for tile in range(columns // TILE):
            cols = pl.ds(tile * TILE, TILE)
            product = mm(left, w_ref[pl.ds(start, plane_rows), cols])
            acc[:, cols] = product if first else acc[:, cols] + product

    def ready(g):
        def one(piece, _):
            mirrored(g, piece)
            return 0

        lax.fori_loop(0, pieces, one, 0)

    def settle(lo, hi):
        start = plane_start(Z - 1)

        def one(piece, _):
            mirrored(Z - 1, piece)
            for core in range(peers):
                cols = pl.ds(pl.multiple_of(core * part + piece * width, width), width)
                product = mm(hidden[:, pl.ds(start, plane_rows)], w_ref[pl.ds(start, plane_rows), cols])
                if Z > 1:
                    product = acc[:, cols] + product
                out_ref[:, cols] = product.astype(jnp.bfloat16)
            return 0

        lax.fori_loop(lo, hi, one, 0)

    def last(lo, hi):
        def one(piece, _):
            stage(Z + 1, piece)
            finish(Z - 1, piece, piece + 1)
            return 0

        lax.fori_loop(lo, hi, one, 0)

    def later(d, _):
        stage_all(d)
        front_all(d)
        return 0

    def middle(g, _):
        finish(g, beside=False, ahead=False)
        ready(g)
        project(g)
        return 0

    def early(g, _):
        finish(g, rest=False)
        return 0

    stage_all(2, pieces // 2, pieces)
    front_all(2)
    if Z > 1:
        finish(0)
        ready(0)
        project(0, first=True)
    lax.fori_loop(3, Z, later, 0)
    if Z > 2:
        lax.fori_loop(1, Z - 2, early, 0)
        finish(Z - 2, rest=False, ahead=False)
    if Z > 2:
        stage_all(Z)
        finish(Z - 2, beside=False)
        lax.fori_loop(1, Z - 2, middle, 0)
    last(0, quarter)
    if Z > 2:
        ready(Z - 2)
        project(Z - 2)
    last(quarter, pieces - quarter)
    settle(0, pieces // 2)

    @pl.when(s < peers - 1)
    def _():
        seg_copy.wait_send()

        def sent(h, _):
            state_copy(h).wait_send()
            return 0

        lax.fori_loop(0, heads, sent, 0)

    if sides:
        bulk(Z * len(sides), side_sem.at[0], recv_sem.at[0]).wait_send()
    if fronts:
        bulk(Z * len(fronts), side_sem.at[1], recv_sem.at[0]).wait_send()

    def sent_plane(plane, _):
        if corners:
            @pl.when(jnp.abs(plane - a) <= reach)
            def _():
                bulk(len(corners), relay_sem.at[plane], recv_sem.at[0]).wait_send()

        for side in (-1, 1):
            away = (a - plane) * side
            on = jnp.logical_and(has[side], away >= 0)

            @pl.when(on)
            def _():
                bulk(1, climb_sem.at[(side + 1) // 2, plane], recv_sem.at[0]).wait_send()

            if corners:
                @pl.when(jnp.logical_and(on, away + 1 > reach_by[side]))
                def _():
                    bulk(len(corners), corner_sem.at[(side + 1) // 2, plane], recv_sem.at[0]).wait_send()

        return 0

    lax.fori_loop(0, Z, sent_plane, 0)
    last(pieces - quarter, pieces)
    settle(pieces // 2, pieces)
    if X * Y * Z > 1:
        for ds in range(1, peers):
            bulk(X * Y * Z - 1, msend.at[ds - 1], recv_sem.at[0]).wait_send()


def local(grid, peers, queries, keys, values, gate_rate, segment_ids, decay_exps, out_weight):
    groups, length, key_features = queries.shape
    heads = decay_exps.shape[0]
    features = values.shape[2]
    columns = out_weight.shape[1]
    chips = grid[0] * grid[1] * grid[2]
    chunk = min(CHUNK, length)
    kw, vw = key_features // heads, features // heads
    bf16, f32 = jnp.bfloat16, jnp.float32
    anywhere = pl.BlockSpec(memory_space=pl.ANY)
    call = pl.pallas_call(
        functools.partial(kernel, grid, peers, heads, chunk, PIECES),
        out_shape=pltpu.VMEM((length, columns), bf16),
        in_specs=[anywhere] * 4
        + [pl.BlockSpec(memory_space=pltpu.VMEM), pl.BlockSpec(memory_space=pltpu.SMEM), anywhere],
        out_specs=pl.BlockSpec(memory_space=pltpu.VMEM),
        scratch_shapes=[
            pltpu.VMEM((length, key_features), bf16),
            pltpu.VMEM((length, key_features), bf16),
            pltpu.VMEM((length, features), bf16),
            pltpu.VMEM((length, key_features), bf16),
            pltpu.VMEM((features, columns), bf16),
            pltpu.VMEM((length, features), bf16),
            pltpu.VMEM((length, columns), f32),
            pltpu.VMEM((1, length), jnp.int32),
            pltpu.VMEM((heads, vw, kw), f32),
            pltpu.VMEM((heads, vw, kw), f32),
            pltpu.SemaphoreType.DMA((5,)),
            pltpu.SemaphoreType.DMA((2,)),
            pltpu.SemaphoreType.DMA((heads,)),
            pltpu.SemaphoreType.DMA((heads,)),
            pltpu.SemaphoreType.DMA((2,)),
            pltpu.SemaphoreType.DMA((grid[0],)),
            pltpu.SemaphoreType.DMA((2, grid[0])),
            pltpu.SemaphoreType.DMA((2, grid[0])),
            pltpu.SemaphoreType.DMA((chips * PIECES,)),
            pltpu.SemaphoreType.DMA((max(peers - 1, 1),)),
            pltpu.SemaphoreType.DMA((max(peers - 1, 1), grid[0] * PIECES)),
        ],
        compiler_params=pltpu.CompilerParams(
            collective_id=0, has_side_effects=True, vmem_limit_bytes=61 * 1024 * 1024
        ),
        name="gla_project",
    )
    outs = [
        call(queries[n], keys[n], values[n], gate_rate[n], segment_ids[n:n + 1], decay_exps, out_weight)
        for n in range(groups)
    ]
    return jnp.stack(outs)


def solution(mesh):
    in_specs = (
        P("batch", "seq", None),
        P("batch", "seq", None),
        P("batch", "seq", None),
        P("batch", "seq", None),
        P("batch", "seq"),
        P(),
        P("batch", None),
    )
    body = functools.partial(local, chip_grid(mesh), mesh.shape["seq"])
    return jax.shard_map(
        body, mesh=mesh, in_specs=in_specs, out_specs=P("batch", "seq", None), check_vma=False
    )
```

```python
import functools
import math

import jax
import jax.numpy as jnp
from jax import lax
from jax.experimental import pallas as pl
from jax.experimental.pallas import tpu as pltpu
from jax.sharding import PartitionSpec as P

MESH = pl.DeviceIdType.MESH
CHUNK = 256
TILE = 512
PIECES = 4


def chip_grid(mesh):
    count = mesh.shape["batch"]
    try:
        axis = mesh.axis_names.index("batch")
        line = mesh.devices.swapaxes(0, axis).reshape(count, -1)[:, 0]
        coords = [tuple(device.coords) for device in line]
        sizes = [len({c[i] for c in coords}) for i in (2, 1, 0)]
        lows = [min(c[i] for c in coords) for i in (2, 1, 0)]
        for index, c in enumerate(coords):
            z, y, x = (c[2] - lows[0], c[1] - lows[1], c[0] - lows[2])
            if (z * sizes[1] + y) * sizes[2] + x != index:
                return (count, 1, 1)
        return tuple(sizes)
    except Exception:
        return (count, 1, 1)


def split(x):
    high = x.astype(jnp.bfloat16)
    return high, (x - high.astype(jnp.float32)).astype(jnp.bfloat16)


def mm(a, b):
    return lax.dot_general(a, b, (((1,), (0,)), ((), ())), preferred_element_type=jnp.float32)


def mm_t(a, b):
    return lax.dot_general(a, b, (((1,), (1,)), ((), ())), preferred_element_type=jnp.float32)


def t_mm(a, b):
    return lax.dot_general(a, b, (((0,), (0,)), ((), ())), preferred_element_type=jnp.float32)


def thresholds(grid):
    Z, Y, X = grid
    beside, corner = X + Y - 2, (X - 1) * (Y - 1)
    picked = []
    for a in range(Z):
        best = None
        for reach in range(Z):
            far = [g for g in range(Z) if abs(g - a) > reach]
            below = a + corner * len([g for g in far if g < a])
            above = Z - 1 - a + corner * len([g for g in far if g > a])
            inside = (Z * beside + (Z - len(far)) * corner) / 2
            load = max(below, above, inside)
            if best is None or load < best[0]:
                best = (load, reach)
        picked.append(best[1])
    return picked


def kernel(
    grid, peers, heads, chunk, pieces,
    q_hbm, k_hbm, v_hbm, g_hbm, seg_ref, exps_ref, w_hbm,
    out_ref,
    q_ref, k_ref, v_ref, g_ref, w_ref, hidden, acc, seg_in, state_in, state_out,
    load_sem, seg_sem, state_send, state_recv, side_sem, relay_sem, climb_sem, corner_sem, recv_sem, msend, mrecv,
):
    Z, Y, X = grid
    s = lax.axis_index("seq")
    me = lax.axis_index("batch")
    length, keys = q_ref.shape
    key_width = keys // heads
    value_width = v_ref.shape[1] // heads
    rows = w_hbm.shape[0]
    columns = w_ref.shape[1]
    part = columns // peers
    width = part // pieces
    plane_rows = rows * X * Y
    a = me // (X * Y)
    swap = X == Y
    nb, nc = X, Y
    sides = [(db, 0) for db in range(1, nb)]
    fronts = [(0, dc) for dc in range(1, nc)]
    corners = [(db, dc) for db in range(1, nb) for dc in range(1, nc)]
    table = thresholds(grid)

    def strides(core):
        if not swap:
            return 1, X
        even = lax.rem(core, 2) == 0
        return jnp.where(even, 1, X), jnp.where(even, X, 1)

    def chip_at(core, plane, db, dc):
        sb, sc = strides(core)
        b = lax.rem(me // sb, nb)
        c = lax.rem(me // sc, nc)
        return (
            plane * (X * Y)
            + lax.rem(b - db + nb, nb) * sb
            + lax.rem(c - dc + nc, nc) * sc
        )

    near = jnp.minimum(a, Z - 1 - a)

    def plane_at(g):
        side = jnp.where(lax.rem(g, 2) == 1, -1, 1)
        rest = jnp.where(a < Z - 1 - a, g, Z - 1 - g)
        return jnp.where(g <= 2 * near, a + (g + 1) // 2 * side, rest)

    def reach_of(plane):
        reach = jnp.int32(table[0])
        for index in range(1, Z):
            reach = jnp.where(plane == index, table[index], reach)
        return reach

    reach = reach_of(a)
    reach_by = {-1: reach_of(a - 1), 1: reach_of(a + 1)}
    has = {-1: a > 0, 1: a < Z - 1}

    def label(plane, db, dc):
        return (plane * nb + db) * nc + dc

    def block(core, start, count, piece, pieces_wide=1):
        return w_ref.at[
            pl.ds(pl.multiple_of(start, rows), count),
            pl.ds(pl.multiple_of(core * part + piece * width, width), pieces_wide * width),
        ]

    def send(held, to, sem, device, piece):
        here = block(s, chip_at(s, *held) * rows, rows, piece)
        return pltpu.make_async_remote_copy(
            src_ref=here, dst_ref=here, send_sem=sem, recv_sem=recv_sem.at[label(*to) * pieces + piece],
            device_id={"batch": device}, device_id_type=MESH,
        )

    def sideways(plane, piece):
        for db, _ in sides:
            send((plane, 0, 0), (plane, db, 0), side_sem.at[0], chip_at(s, a, -db, 0), piece).start()

    def forwards(plane, piece):
        for _, dc in fronts:
            send((plane, 0, 0), (plane, 0, dc), side_sem.at[1], chip_at(s, a, 0, -dc), piece).start()

    def climb(plane, side, piece):
        to = (plane, 0, 0)
        send(to, to, climb_sem.at[(side + 1) // 2, plane], me + side * X * Y, piece).start()

    def climb_corners(plane, side, piece):
        for corner in corners:
            to = (plane, *corner)
            send(to, to, corner_sem.at[(side + 1) // 2, plane], me + side * X * Y, piece).start()

    def wait_piece(plane, db, dc, piece):
        to = (plane, db, dc)
        send(to, to, side_sem.at[0], lax.rem(me + 1, X * Y * Z), piece).wait_recv()

    def share(plane, db, dc, piece):
        here = block(s, chip_at(s, plane, db, dc) * rows, rows, piece)
        for ds in range(1, peers):
            pltpu.make_async_remote_copy(
                src_ref=here, dst_ref=here,
                send_sem=msend.at[ds - 1], recv_sem=mrecv.at[ds - 1, plane * pieces + piece],
                device_id={"seq": lax.rem(s + ds, peers)}, device_id_type=MESH,
            ).start()

    def bulk(count, send_end, recv_end, core=0, piece=0, pieces_wide=pieces):
        here = block(core, 0, count * rows, piece, pieces_wide)
        return pltpu.make_async_remote_copy(
            src_ref=here, dst_ref=here, send_sem=send_end, recv_sem=recv_end,
            device_id={"batch": lax.rem(me + 1, X * Y * Z)}, device_id_type=MESH,
        )

    def inside(plane):
        return jnp.logical_and(plane >= 0, plane < Z)

    def needs(distance, side):
        return jnp.logical_and(has[side], distance + 1 > reach_by[side])

    def stage(d, piece):
        for side in (-1, 1):
            plane = a + side * d

            @pl.when(inside(plane))
            def _():
                wait_piece(plane, 0, 0, piece)
                pl.when(has[-side])(lambda: climb(plane, -side, piece))
                pl.when(d < Z - 1)(lambda: sideways(plane, piece))
                share(plane, 0, 0, piece)

        @pl.when(d == 1)
        def _():
            for db, _ in sides:
                wait_piece(a, db, 0, piece)
                for _, dc in fronts:
                    send((a, db, 0), (a, db, dc), relay_sem.at[a], chip_at(s, a, 0, -dc), piece).start()
                share(a, db, 0, piece)

        if not corners:
            return

        f = d - 2
        for side in (-1, 1):
            plane = a + side * f

            @pl.when(jnp.logical_and(jnp.logical_and(f > 0, f <= reach), inside(plane)))
            def _():
                for _, dc in fronts:
                    wait_piece(plane, 0, dc, piece)
                    for db, _ in sides:
                        send(
                            (plane, 0, dc), (plane, db, dc), relay_sem.at[plane],
                            chip_at(s, a, -db, 0), piece,
                        ).start()
                    share(plane, 0, dc, piece)

        def corner_step(plane, distance, side, both):
            for corner in corners:
                wait_piece(plane, *corner, piece)
            pl.when(needs(distance, -side))(lambda: climb_corners(plane, -side, piece))
            if both:
                pl.when(needs(distance, side))(lambda: climb_corners(plane, side, piece))
            for corner in corners:
                share(plane, *corner, piece)

        pl.when(d == 2)(lambda: corner_step(a, 0, -1, True))
        for side in (-1, 1):
            late = a + side * (d - 3)
            on = jnp.logical_and(jnp.logical_and(d > 3, d - 3 <= reach), needs(d - 3, -side))
            pl.when(jnp.logical_and(on, inside(late)))(lambda: corner_step(late, d - 3, side, False))
        for side in (-1, 1):
            far = a + side * f
            on = jnp.logical_and(jnp.logical_and(f > 0, f > reach), inside(far))
            pl.when(on)(lambda: corner_step(far, f, side, False))

    def stage_all(d, lo=0, hi=pieces):
        def one(piece, _):
            stage(d, piece)
            return 0

        lax.fori_loop(lo, hi, one, 0)

    def front_all(d):
        def one(piece, _):
            for side in (-1, 1):
                plane = a + side * d

                @pl.when(inside(plane))
                def _():
                    pl.when(d == Z - 1)(lambda: sideways(plane, piece))
                    forwards(plane, piece)
            return 0

        lax.fori_loop(0, pieces, one, 0)

    def finish(g, lo=0, hi=pieces, beside=True, rest=True, ahead=True):
        plane = plane_at(g)
        distance = jnp.abs(plane - a)
        side = jnp.where(plane < a, -1, 1)
        onward = jnp.where(side < 0, needs(distance, 1), needs(distance, -1))
        near_by = distance <= reach

        def one(piece, _):
            if beside:
                for db, _ in sides:
                    @pl.when(distance > 0)
                    def _():
                        wait_piece(plane, db, 0, piece)
                        share(plane, db, 0, piece)

            if ahead:
                for _, dc in fronts:
                    @pl.when(jnp.logical_or(distance == 0, jnp.logical_not(near_by)) if corners else distance >= 0)
                    def _():
                        wait_piece(plane, 0, dc, piece)
                        share(plane, 0, dc, piece)

            if corners and rest:
                late = jnp.logical_and(near_by, jnp.logical_not(onward))

                @pl.when(jnp.logical_and(late, distance > 0))
                def _():
                    for corner in corners:
                        wait_piece(plane, *corner, piece)
                        share(plane, *corner, piece)
            return 0

        lax.fori_loop(lo, hi, one, 0)

    def mirrored(g, piece):
        plane = plane_at(g)
        for ds in range(1, peers):
            core = lax.rem(s - ds + peers, peers)
            count = X * Y - 1 if isinstance(g, int) and g == 0 else X * Y
            if count:
                bulk(
                    count, msend.at[ds - 1], mrecv.at[ds - 1, plane * pieces + piece], core, piece, 1
                ).wait_recv()

    loads = [
        pltpu.make_async_copy(
            w_hbm, w_ref.at[pl.ds(pl.multiple_of(me * rows, rows), rows), :], load_sem.at[0]
        ),
        pltpu.make_async_copy(g_hbm, g_ref, load_sem.at[1]),
        pltpu.make_async_copy(k_hbm, k_ref, load_sem.at[2]),
        pltpu.make_async_copy(q_hbm, q_ref, load_sem.at[3]),
        pltpu.make_async_copy(v_hbm, v_ref, load_sem.at[4]),
    ]
    for load in loads:
        load.start()

    barrier = pltpu.get_barrier_semaphore()
    friends = [{"batch": chip_at(s, a, d, 0)} for d in range(1, nb)]
    friends += [{"batch": chip_at(s, a, 0, d)} for d in range(1, nc)]
    friends += [{"seq": lax.rem(s + d, peers)} for d in range(1, peers)]
    for friend in friends:
        pl.semaphore_signal(barrier, inc=1, device_id=friend, device_id_type=MESH)

    @pl.when(a < Z - 1)
    def _():
        pl.semaphore_signal(barrier, inc=1, device_id={"batch": me + X * Y}, device_id_type=MESH)

    @pl.when(a > 0)
    def _():
        pl.semaphore_signal(barrier, inc=1, device_id={"batch": me - X * Y}, device_id_type=MESH)

    above, below = jnp.where(a < Z - 1, 1, 0), jnp.where(a > 0, 1, 0)
    pl.semaphore_wait(barrier, len(friends) + above + below)

    loads[0].wait()

    def own(piece, _):
        for side in (-1, 1):
            pl.when(has[side])(lambda: climb(a, side, piece))
        sideways(a, piece)
        forwards(a, piece)
        return 0

    lax.fori_loop(0, pieces, own, 0)

    def next_core():
        return {"seq": lax.rem(s + 1, peers)}

    seg_copy = pltpu.make_async_remote_copy(
        src_ref=seg_ref, dst_ref=seg_in, send_sem=seg_sem.at[0], recv_sem=seg_sem.at[1],
        device_id=next_core(), device_id_type=MESH,
    )

    def state_copy(h):
        return pltpu.make_async_remote_copy(
            src_ref=state_out.at[h], dst_ref=state_in.at[h],
            send_sem=state_send.at[h], recv_sem=state_recv.at[h],
            device_id=next_core(), device_id_type=MESH,
        )

    @pl.when(s < peers - 1)
    def _():
        seg_copy.start()

    @pl.when(s == 0)
    def _():
        state_in[...] = jnp.zeros_like(state_in)
        seg_in[...] = jnp.full(seg_in.shape, -1, jnp.int32)

    for load in loads[1:]:
        load.wait()

    @pl.when(s > 0)
    def _():
        seg_copy.wait_recv()

    order_t = lax.broadcasted_iota(jnp.int32, (chunk, chunk), 0)
    order_s = lax.broadcasted_iota(jnp.int32, (chunk, chunk), 1)
    causal = order_t >= order_s
    triangle = jnp.where(causal, 1.0, 0.0).astype(jnp.bfloat16)
    seg_row = seg_ref[...].astype(jnp.float32)
    before = seg_in[...].astype(jnp.float32)[:, length - 1:]
    seg_wide = jnp.broadcast_to(seg_row, (128, length)).T

    quarter = pieces // 4

    def first():
        stage_all(1, 0, quarter)

    def second():
        stage_all(1, quarter, pieces - quarter)

    def third():
        stage_all(1, pieces - quarter, pieces)
        front_all(1)

    def fourth():
        stage_all(2, 0, pieces // 2)

    events = [first, second, third, fourth]
    lead = jnp.where(s == 0, 2, 0)

    def head(h, _):
        for number, event in enumerate(events):
            pl.when(h - lead == number)(event)

        exponent = jnp.full((1, key_width), exps_ref[h], jnp.int32).astype(jnp.float32)
        scale = jnp.exp2(-exponent) * (-1.0 / 16.0)

        @pl.when(s > 0)
        def _():
            state_copy(h).wait_recv()

        state = state_in[h]
        previous = before
        key_cols = pl.ds(pl.multiple_of(h * key_width, key_width), key_width)
        value_cols = pl.ds(pl.multiple_of(h * value_width, value_width), value_width)
        for i in range(length // chunk):
            now = pl.ds(i * chunk, chunk)
            log = mm(triangle, g_ref[now, key_cols]) * scale
            fall = jnp.exp(log)
            raised_q = q_ref[now, key_cols].astype(jnp.float32) * (fall * (1.0 / math.sqrt(key_width)))
            raised_k = k_ref[now, key_cols].astype(jnp.float32) * jnp.exp(-log)
            value = v_ref[now, value_cols]
            q_hi, q_lo = split(raised_q)
            k_hi, k_lo = split(raised_k)
            row = seg_row[:, i * chunk:(i + 1) * chunk]
            column = seg_wide[i * chunk:(i + 1) * chunk, :1]
            scores = mm_t(q_hi, k_hi) + mm_t(q_hi, k_lo) + mm_t(q_lo, k_hi)
            scores = jnp.where(jnp.logical_and(causal, column == row), scores, 0.0)
            p_hi, p_lo = split(scores)
            s_hi, s_lo = split(state)
            carried = mm_t(q_hi, s_hi) + mm_t(q_hi, s_lo) + mm_t(q_lo, s_hi)
            mixed = mm(p_hi, value) + mm(p_lo, value)
            mixed = mixed + jnp.where(column == previous, carried, 0.0)
            power = jnp.mean(mixed * mixed, axis=-1, keepdims=True)
            hidden[now, value_cols] = (mixed * lax.rsqrt(power + 1.0)).astype(jnp.bfloat16)
            final = fall[chunk - 1:, :]
            last = row[:, chunk - 1:]
            weighted = jnp.where(column == last, raised_k * final, 0.0)
            w_hi, w_lo = split(weighted)
            kept = jnp.where(last == previous, state * final, 0.0)
            state = kept + t_mm(value, w_hi) + t_mm(value, w_lo)
            previous = last

        @pl.when(s < peers - 1)
        def _():
            state_out[h] = state
            state_copy(h).start()

        return 0

    lax.fori_loop(0, heads, head, 0)
    for number, event in enumerate(events):
        pl.when(heads - lead <= number)(event)

    def plane_start(g):
        return pl.multiple_of(plane_at(g) * plane_rows, plane_rows)

    def add(g, cols, first, final):
        start = plane_start(g)
        product = mm(hidden[:, pl.ds(start, plane_rows)], w_ref[pl.ds(start, plane_rows), cols])
        if not first:
            product = acc[:, cols] + product
        if final:
            out_ref[:, cols] = product.astype(jnp.bfloat16)
        else:
            acc[:, cols] = product

    def project(g):
        for tile in range(columns // TILE):
            add(g, pl.ds(tile * TILE, TILE), False, False)

    def settle(g, piece, final=False):
        mirrored(g, piece)
        for core in range(peers):
            cols = pl.ds(pl.multiple_of(core * part + piece * width, width), width)
            add(g, cols, isinstance(g, int) and g == 0, final)

    def loop(lo, hi, body):
        def one(index, _):
            body(index)
            return 0

        lax.fori_loop(lo, hi, one, 0)

    def later(d):
        stage_all(d)
        front_all(d)

    def middle(g):
        finish(g, beside=False, ahead=False)
        loop(0, pieces, lambda piece: mirrored(g, piece))
        project(g)

    def opening(piece):
        stage(3, piece)
        settle(0, piece)

    def tidy(piece):
        finish(Z - 2, piece, piece + 1, beside=False)
        if Z > 3:
            finish(Z - 3, piece, piece + 1, beside=False, ahead=False)

    def streaming(piece):
        stage(Z, piece)

        @pl.when(piece > 0)
        def _():
            tidy(piece - 1)

        @pl.when(piece > 1)
        def _():
            stream(piece - 2)

    def stream(piece):
        for g in range(max(Z - 3, 1), Z - 1):
            settle(g, piece)

    def closing(piece):
        stage(Z + 1, piece)
        finish(Z - 1, piece, piece + 1)

        @pl.when(piece > 0)
        def _():
            settle(Z - 1, piece - 1, final=True)

    stage_all(2, pieces // 2, pieces)
    front_all(2)
    finish(0)
    if Z > 3:
        loop(0, pieces, opening)
        front_all(3)
        loop(4, Z, later)
    elif Z > 1:
        loop(0, pieces, lambda piece: settle(0, piece))
    if Z > 2:
        loop(1, Z - 2, lambda g: finish(g, rest=False))
        finish(Z - 2, rest=False, ahead=False)
        loop(1, Z - 3, middle)
        loop(0, pieces, streaming)
        tidy(pieces - 1)
        loop(max(pieces - 2, 0), pieces, stream)
    if Z > 1:
        loop(0, pieces, closing)

    @pl.when(s < peers - 1)
    def _():
        seg_copy.wait_send()

        def sent(h, _):
            state_copy(h).wait_send()
            return 0

        lax.fori_loop(0, heads, sent, 0)

    if sides:
        bulk(Z * len(sides), side_sem.at[0], recv_sem.at[0]).wait_send()
    if fronts:
        bulk(Z * len(fronts), side_sem.at[1], recv_sem.at[0]).wait_send()

    def sent_plane(plane, _):
        if corners:
            @pl.when(jnp.abs(plane - a) <= reach)
            def _():
                bulk(len(corners), relay_sem.at[plane], recv_sem.at[0]).wait_send()

        for side in (-1, 1):
            away = (a - plane) * side
            on = jnp.logical_and(has[side], away >= 0)

            @pl.when(on)
            def _():
                bulk(1, climb_sem.at[(side + 1) // 2, plane], recv_sem.at[0]).wait_send()

            if corners:
                @pl.when(jnp.logical_and(on, away + 1 > reach_by[side]))
                def _():
                    bulk(len(corners), corner_sem.at[(side + 1) // 2, plane], recv_sem.at[0]).wait_send()

        return 0

    lax.fori_loop(0, Z, sent_plane, 0)
    if Z > 1:
        settle(Z - 1, pieces - 1, final=True)
    else:
        loop(0, pieces, lambda piece: settle(0, piece, final=True))
    if X * Y * Z > 1:
        for ds in range(1, peers):
            bulk(X * Y * Z - 1, msend.at[ds - 1], recv_sem.at[0]).wait_send()


def local(grid, peers, queries, keys, values, gate_rate, segment_ids, decay_exps, out_weight):
    groups, length, key_features = queries.shape
    heads = decay_exps.shape[0]
    features = values.shape[2]
    columns = out_weight.shape[1]
    chips = grid[0] * grid[1] * grid[2]
    chunk = min(CHUNK, length)
    kw, vw = key_features // heads, features // heads
    bf16, f32 = jnp.bfloat16, jnp.float32
    anywhere = pl.BlockSpec(memory_space=pl.ANY)
    call = pl.pallas_call(
        functools.partial(kernel, grid, peers, heads, chunk, PIECES),
        out_shape=pltpu.VMEM((length, columns), bf16),
        in_specs=[anywhere] * 4
        + [pl.BlockSpec(memory_space=pltpu.VMEM), pl.BlockSpec(memory_space=pltpu.SMEM), anywhere],
        out_specs=pl.BlockSpec(memory_space=pltpu.VMEM),
        scratch_shapes=[
            pltpu.VMEM((length, key_features), bf16),
            pltpu.VMEM((length, key_features), bf16),
            pltpu.VMEM((length, features), bf16),
            pltpu.VMEM((length, key_features), bf16),
            pltpu.VMEM((features, columns), bf16),
            pltpu.VMEM((length, features), bf16),
            pltpu.VMEM((length, columns), f32),
            pltpu.VMEM((1, length), jnp.int32),
            pltpu.VMEM((heads, vw, kw), f32),
            pltpu.VMEM((heads, vw, kw), f32),
            pltpu.SemaphoreType.DMA((5,)),
            pltpu.SemaphoreType.DMA((2,)),
            pltpu.SemaphoreType.DMA((heads,)),
            pltpu.SemaphoreType.DMA((heads,)),
            pltpu.SemaphoreType.DMA((2,)),
            pltpu.SemaphoreType.DMA((grid[0],)),
            pltpu.SemaphoreType.DMA((2, grid[0])),
            pltpu.SemaphoreType.DMA((2, grid[0])),
            pltpu.SemaphoreType.DMA((chips * PIECES,)),
            pltpu.SemaphoreType.DMA((max(peers - 1, 1),)),
            pltpu.SemaphoreType.DMA((max(peers - 1, 1), grid[0] * PIECES)),
        ],
        compiler_params=pltpu.CompilerParams(
            collective_id=0, has_side_effects=True, vmem_limit_bytes=61 * 1024 * 1024
        ),
        name="gla_project",
    )
    outs = [
        call(queries[n], keys[n], values[n], gate_rate[n], segment_ids[n:n + 1], decay_exps, out_weight)
        for n in range(groups)
    ]
    return jnp.stack(outs)


def solution(mesh):
    in_specs = (
        P("batch", "seq", None),
        P("batch", "seq", None),
        P("batch", "seq", None),
        P("batch", "seq", None),
        P("batch", "seq"),
        P(),
        P("batch", None),
    )
    body = functools.partial(local, chip_grid(mesh), mesh.shape["seq"])
    return jax.shard_map(
        body, mesh=mesh, in_specs=in_specs, out_specs=P("batch", "seq", None), check_vma=False
    )
```

```python
import functools
import math

import jax
import jax.numpy as jnp
from jax import lax
from jax.experimental import pallas as pl
from jax.experimental.pallas import tpu as pltpu
from jax.sharding import PartitionSpec as P

MESH = pl.DeviceIdType.MESH
CHUNK = 256
TILE = 512
PIECES = 4
OPENING = [(1, (0, 1)), (2, (1, 4)), (3, (4, 5))]
CLOSING = [(0, (5, 6)), (1, (6, 7)), (2, (7, 8))]


def chip_grid(mesh):
    count = mesh.shape["batch"]
    try:
        axis = mesh.axis_names.index("batch")
        line = mesh.devices.swapaxes(0, axis).reshape(count, -1)[:, 0]
        coords = [tuple(device.coords) for device in line]
        sizes = [len({c[i] for c in coords}) for i in (2, 1, 0)]
        lows = [min(c[i] for c in coords) for i in (2, 1, 0)]
        for index, c in enumerate(coords):
            z, y, x = (c[2] - lows[0], c[1] - lows[1], c[0] - lows[2])
            if (z * sizes[1] + y) * sizes[2] + x != index:
                return (count, 1, 1)
        return tuple(sizes)
    except Exception:
        return (count, 1, 1)


def split(x):
    high = x.astype(jnp.bfloat16)
    return high, (x - high.astype(jnp.float32)).astype(jnp.bfloat16)


def mm(a, b):
    return lax.dot_general(a, b, (((1,), (0,)), ((), ())), preferred_element_type=jnp.float32)


def mm_t(a, b):
    return lax.dot_general(a, b, (((1,), (1,)), ((), ())), preferred_element_type=jnp.float32)


def t_mm(a, b):
    return lax.dot_general(a, b, (((0,), (0,)), ((), ())), preferred_element_type=jnp.float32)


def thresholds(grid):
    Z, Y, X = grid
    beside, corner = X + Y - 2, (X - 1) * (Y - 1)
    picked = []
    for a in range(Z):
        best = None
        for reach in range(Z):
            far = [g for g in range(Z) if abs(g - a) > reach]
            below = a + corner * len([g for g in far if g < a])
            above = Z - 1 - a + corner * len([g for g in far if g > a])
            inside = (Z * beside + (Z - len(far)) * corner) / 2
            load = max(below, above, inside)
            if best is None or load < best[0]:
                best = (load, reach)
        picked.append(best[1])
    return picked


def kernel(
    grid, peers, heads, chunk, pieces,
    q_hbm, k_hbm, v_hbm, g_hbm, seg_ref, exps_ref, w_hbm,
    out_ref,
    q_ref, k_ref, v_ref, g_ref, w_ref, hidden, acc, mixed, seg_in, state_in, state_out,
    load_sem, seg_sem, state_send, state_recv, side_sem, relay_sem, climb_sem, corner_sem, recv_sem, msend, mrecv,
):
    Z, Y, X = grid
    s = lax.axis_index("seq")
    me = lax.axis_index("batch")
    length, keys = q_ref.shape
    key_width = keys // heads
    value_width = v_ref.shape[1] // heads
    rows = w_hbm.shape[0]
    columns = w_ref.shape[1]
    part = columns // peers
    width = part // pieces
    plane_rows = rows * X * Y
    a = me // (X * Y)
    swap = X == Y
    nb, nc = X, Y
    sides = [(db, 0) for db in range(1, nb)]
    fronts = [(0, dc) for dc in range(1, nc)]
    corners = [(db, dc) for db in range(1, nb) for dc in range(1, nc)]
    table = thresholds(grid)

    def strides(core):
        if not swap:
            return 1, X
        even = lax.rem(core, 2) == 0
        return jnp.where(even, 1, X), jnp.where(even, X, 1)

    def chip_at(core, plane, db, dc):
        sb, sc = strides(core)
        b = lax.rem(me // sb, nb)
        c = lax.rem(me // sc, nc)
        return (
            plane * (X * Y)
            + lax.rem(b - db + nb, nb) * sb
            + lax.rem(c - dc + nc, nc) * sc
        )

    near = jnp.minimum(a, Z - 1 - a)

    def plane_at(g):
        side = jnp.where(lax.rem(g, 2) == 1, -1, 1)
        rest = jnp.where(a < Z - 1 - a, g, Z - 1 - g)
        return jnp.where(g <= 2 * near, a + (g + 1) // 2 * side, rest)

    def reach_of(plane):
        reach = jnp.int32(table[0])
        for index in range(1, Z):
            reach = jnp.where(plane == index, table[index], reach)
        return reach

    reach = reach_of(a)
    reach_by = {-1: reach_of(a - 1), 1: reach_of(a + 1)}
    has = {-1: a > 0, 1: a < Z - 1}

    def label(plane, db, dc):
        return (plane * nb + db) * nc + dc

    def block(core, start, count, piece, pieces_wide=1):
        return w_ref.at[
            pl.ds(pl.multiple_of(start, rows), count),
            pl.ds(pl.multiple_of(core * part + piece * width, width), pieces_wide * width),
        ]

    def send(held, to, sem, device, piece):
        here = block(s, chip_at(s, *held) * rows, rows, piece)
        return pltpu.make_async_remote_copy(
            src_ref=here, dst_ref=here, send_sem=sem, recv_sem=recv_sem.at[label(*to) * pieces + piece],
            device_id={"batch": device}, device_id_type=MESH,
        )

    def sideways(plane, piece):
        for db, _ in sides:
            send((plane, 0, 0), (plane, db, 0), side_sem.at[0], chip_at(s, a, -db, 0), piece).start()

    def forwards(plane, piece):
        for _, dc in fronts:
            send((plane, 0, 0), (plane, 0, dc), side_sem.at[1], chip_at(s, a, 0, -dc), piece).start()

    def climb(plane, side, piece):
        to = (plane, 0, 0)
        send(to, to, climb_sem.at[(side + 1) // 2, plane], me + side * X * Y, piece).start()

    def climb_corners(plane, side, piece):
        for corner in corners:
            to = (plane, *corner)
            send(to, to, corner_sem.at[(side + 1) // 2, plane], me + side * X * Y, piece).start()

    def wait_piece(plane, db, dc, piece):
        to = (plane, db, dc)
        send(to, to, side_sem.at[0], lax.rem(me + 1, X * Y * Z), piece).wait_recv()

    def share(plane, db, dc, piece):
        here = block(s, chip_at(s, plane, db, dc) * rows, rows, piece)
        for ds in range(1, peers):
            pltpu.make_async_remote_copy(
                src_ref=here, dst_ref=here,
                send_sem=msend.at[ds - 1], recv_sem=mrecv.at[ds - 1, plane * pieces + piece],
                device_id={"seq": lax.rem(s + ds, peers)}, device_id_type=MESH,
            ).start()

    def bulk(count, send_end, recv_end, core=0, piece=0, pieces_wide=pieces):
        here = block(core, 0, count * rows, piece, pieces_wide)
        return pltpu.make_async_remote_copy(
            src_ref=here, dst_ref=here, send_sem=send_end, recv_sem=recv_end,
            device_id={"batch": lax.rem(me + 1, X * Y * Z)}, device_id_type=MESH,
        )

    def inside(plane):
        return jnp.logical_and(plane >= 0, plane < Z)

    def needs(distance, side):
        return jnp.logical_and(has[side], distance + 1 > reach_by[side])

    def stage(d, piece):
        for side in (-1, 1):
            plane = a + side * d

            @pl.when(inside(plane))
            def _():
                wait_piece(plane, 0, 0, piece)
                pl.when(has[-side])(lambda: climb(plane, -side, piece))
                pl.when(d < Z - 1)(lambda: sideways(plane, piece))
                share(plane, 0, 0, piece)

        @pl.when(d == 1)
        def _():
            for db, _ in sides:
                wait_piece(a, db, 0, piece)
                for _, dc in fronts:
                    send((a, db, 0), (a, db, dc), relay_sem.at[a], chip_at(s, a, 0, -dc), piece).start()
                share(a, db, 0, piece)

        if not corners:
            return

        f = d - 2
        for side in (-1, 1):
            plane = a + side * f

            @pl.when(jnp.logical_and(jnp.logical_and(f > 0, f <= reach), inside(plane)))
            def _():
                for _, dc in fronts:
                    wait_piece(plane, 0, dc, piece)
                    for db, _ in sides:
                        send(
                            (plane, 0, dc), (plane, db, dc), relay_sem.at[plane],
                            chip_at(s, a, -db, 0), piece,
                        ).start()
                    share(plane, 0, dc, piece)

        def corner_step(plane, distance, side, both):
            for corner in corners:
                wait_piece(plane, *corner, piece)
            pl.when(needs(distance, -side))(lambda: climb_corners(plane, -side, piece))
            if both:
                pl.when(needs(distance, side))(lambda: climb_corners(plane, side, piece))
            for corner in corners:
                share(plane, *corner, piece)

        pl.when(d == 2)(lambda: corner_step(a, 0, -1, True))
        for side in (-1, 1):
            late = a + side * (d - 3)
            on = jnp.logical_and(jnp.logical_and(d > 3, d - 3 <= reach), needs(d - 3, -side))
            pl.when(jnp.logical_and(on, inside(late)))(lambda: corner_step(late, d - 3, side, False))
        for side in (-1, 1):
            far = a + side * f
            on = jnp.logical_and(jnp.logical_and(f > 0, f > reach), inside(far))
            pl.when(on)(lambda: corner_step(far, f, side, False))

    def stage_all(d, lo=0, hi=pieces):
        def one(piece, _):
            stage(d, piece)
            return 0

        lax.fori_loop(lo, hi, one, 0)

    def front_all(d):
        def one(piece, _):
            for side in (-1, 1):
                plane = a + side * d

                @pl.when(inside(plane))
                def _():
                    pl.when(d == Z - 1)(lambda: sideways(plane, piece))
                    forwards(plane, piece)
            return 0

        lax.fori_loop(0, pieces, one, 0)

    def finish(g, lo=0, hi=pieces, beside=True, rest=True, ahead=True):
        plane = plane_at(g)
        distance = jnp.abs(plane - a)
        side = jnp.where(plane < a, -1, 1)
        onward = jnp.where(side < 0, needs(distance, 1), needs(distance, -1))
        near_by = distance <= reach

        def one(piece, _):
            if beside:
                for db, _ in sides:
                    @pl.when(distance > 0)
                    def _():
                        wait_piece(plane, db, 0, piece)
                        share(plane, db, 0, piece)

            if ahead:
                for _, dc in fronts:
                    @pl.when(jnp.logical_or(distance == 0, jnp.logical_not(near_by)) if corners else distance >= 0)
                    def _():
                        wait_piece(plane, 0, dc, piece)
                        share(plane, 0, dc, piece)

            if corners and rest:
                late = jnp.logical_and(near_by, jnp.logical_not(onward))

                @pl.when(jnp.logical_and(late, distance > 0))
                def _():
                    for corner in corners:
                        wait_piece(plane, *corner, piece)
                        share(plane, *corner, piece)
            return 0

        lax.fori_loop(lo, hi, one, 0)

    def mirrored(g, piece):
        plane = plane_at(g)
        for ds in range(1, peers):
            core = lax.rem(s - ds + peers, peers)
            count = X * Y - 1 if isinstance(g, int) and g == 0 else X * Y
            if count:
                bulk(
                    count, msend.at[ds - 1], mrecv.at[ds - 1, plane * pieces + piece], core, piece, 1
                ).wait_recv()

    loads = [
        pltpu.make_async_copy(
            w_hbm, w_ref.at[pl.ds(pl.multiple_of(me * rows, rows), rows), :], load_sem.at[0]
        ),
        pltpu.make_async_copy(g_hbm, g_ref, load_sem.at[1]),
        pltpu.make_async_copy(k_hbm, k_ref, load_sem.at[2]),
        pltpu.make_async_copy(q_hbm, q_ref, load_sem.at[3]),
        pltpu.make_async_copy(v_hbm, v_ref, load_sem.at[4]),
    ]
    for load in loads:
        load.start()

    barrier = pltpu.get_barrier_semaphore()
    friends = [{"batch": chip_at(s, a, d, 0)} for d in range(1, nb)]
    friends += [{"batch": chip_at(s, a, 0, d)} for d in range(1, nc)]
    friends += [{"seq": lax.rem(s + d, peers)} for d in range(1, peers)]
    for friend in friends:
        pl.semaphore_signal(barrier, inc=1, device_id=friend, device_id_type=MESH)

    @pl.when(a < Z - 1)
    def _():
        pl.semaphore_signal(barrier, inc=1, device_id={"batch": me + X * Y}, device_id_type=MESH)

    @pl.when(a > 0)
    def _():
        pl.semaphore_signal(barrier, inc=1, device_id={"batch": me - X * Y}, device_id_type=MESH)

    above, below = jnp.where(a < Z - 1, 1, 0), jnp.where(a > 0, 1, 0)
    pl.semaphore_wait(barrier, len(friends) + above + below)

    loads[0].wait()

    def own(piece, _):
        for side in (-1, 1):
            pl.when(has[side])(lambda: climb(a, side, piece))
        sideways(a, piece)
        forwards(a, piece)
        return 0

    lax.fori_loop(0, pieces, own, 0)

    def next_core():
        return {"seq": lax.rem(s + 1, peers)}

    seg_copy = pltpu.make_async_remote_copy(
        src_ref=seg_ref, dst_ref=seg_in, send_sem=seg_sem.at[0], recv_sem=seg_sem.at[1],
        device_id=next_core(), device_id_type=MESH,
    )

    def state_copy(h):
        return pltpu.make_async_remote_copy(
            src_ref=state_out.at[h], dst_ref=state_in.at[h],
            send_sem=state_send.at[h], recv_sem=state_recv.at[h],
            device_id=next_core(), device_id_type=MESH,
        )

    @pl.when(s < peers - 1)
    def _():
        seg_copy.start()

    @pl.when(s == 0)
    def _():
        seg_in[...] = jnp.full(seg_in.shape, -1, jnp.int32)

    for load in loads[1:]:
        load.wait()

    @pl.when(s > 0)
    def _():
        seg_copy.wait_recv()

    order_t = lax.broadcasted_iota(jnp.int32, (chunk, chunk), 0)
    order_s = lax.broadcasted_iota(jnp.int32, (chunk, chunk), 1)
    causal = order_t >= order_s
    triangle = jnp.where(causal, 1.0, 0.0).astype(jnp.bfloat16)
    seg_row = seg_ref[...].astype(jnp.float32)
    before = seg_in[...].astype(jnp.float32)[:, length - 1:]
    seg_wide = jnp.broadcast_to(seg_row, (128, length)).T

    def relay_steps(lo, hi):
        def one(number, _):
            stage(1 + number // pieces, lax.rem(number, pieces))
            pl.when(number == pieces - 1)(lambda: front_all(1))
            return 0

        lax.fori_loop(lo, hi, one, 0)

    def relays_at(h, plan):
        lo = hi = 0
        for at, (start, stop) in plan:
            lo, hi = jnp.where(h == at, start, lo), jnp.where(h == at, stop, hi)
        relay_steps(lo, hi)

    planned = heads == 4 and pieces == 4

    def columns_of(h):
        key_cols = pl.ds(pl.multiple_of(h * key_width, key_width), key_width)
        return key_cols, pl.ds(pl.multiple_of(h * value_width, value_width), value_width)

    def head(h, _):
        relays_at(h, OPENING if planned else [])

        exponent = jnp.full((1, key_width), exps_ref[h], jnp.int32).astype(jnp.float32)
        scale = jnp.exp2(-exponent) * (-1.0 / 16.0)
        key_cols, value_cols = columns_of(h)
        state = previous = offset = None
        for i in range(length // chunk):
            now = pl.ds(i * chunk, chunk)
            log = mm(triangle, g_ref[now, key_cols]) * scale
            fall = jnp.exp(log)
            raised_q = q_ref[now, key_cols].astype(jnp.float32) * (fall * (1.0 / math.sqrt(key_width)))
            raised_k = k_ref[now, key_cols].astype(jnp.float32) * jnp.exp(-log)
            value = v_ref[now, value_cols]
            q_hi, q_lo = split(raised_q)
            k_hi, k_lo = split(raised_k)
            row = seg_row[:, i * chunk:(i + 1) * chunk]
            column = seg_wide[i * chunk:(i + 1) * chunk, :1]
            scores = mm_t(q_hi, k_hi) + mm_t(q_hi, k_lo) + mm_t(q_lo, k_hi)
            scores = jnp.where(jnp.logical_and(causal, column == row), scores, 0.0)
            p_hi, p_lo = split(scores)
            inner = mm(p_hi, value) + mm(p_lo, value)
            if i > 0:
                s_hi, s_lo = split(state)
                carried = mm_t(q_hi, s_hi) + mm_t(q_hi, s_lo) + mm_t(q_lo, s_hi)
                inner = inner + jnp.where(column == previous, carried, 0.0)
            mixed[now, value_cols] = inner
            if peers > 1:
                whole = raised_q if i == 0 else raised_q * jnp.exp(offset)
                q_ref[now, key_cols], g_ref[now, key_cols] = split(whole)
            final = fall[chunk - 1:, :]
            end = log[chunk - 1:, :]
            offset = end if i == 0 else offset + end
            last = row[:, chunk - 1:]
            weighted = jnp.where(column == last, raised_k * final, 0.0)
            w_hi, w_lo = split(weighted)
            grown = t_mm(value, w_hi) + t_mm(value, w_lo)
            state = grown if i == 0 else grown + jnp.where(last == previous, state * final, 0.0)
            previous = last

        if peers > 1:
            @pl.when(s == 0)
            def _():
                state_out[h] = state
                state_copy(h).start()

        if peers > 2:
            @pl.when(jnp.logical_and(s > 0, s < peers - 1))
            def _():
                state_copy(h).wait_recv()
                state_out[h] = state + jnp.where(previous == before, state_in[h] * jnp.exp(offset), 0.0)
                state_copy(h).start()

        return 0

    def close(h, carry):
        key_cols, value_cols = columns_of(h)
        if carry:
            if peers > 2:
                pl.when(s == peers - 1)(lambda: state_copy(h).wait_recv())
            else:
                state_copy(h).wait_recv()
            s_hi, s_lo = split(state_in[h])
        for i in range(length // chunk):
            now = pl.ds(i * chunk, chunk)
            total = mixed[now, value_cols]
            if carry:
                q_hi, q_lo = q_ref[now, key_cols], g_ref[now, key_cols]
                carried = mm_t(q_hi, s_hi) + mm_t(q_hi, s_lo) + mm_t(q_lo, s_hi)
                column = seg_wide[i * chunk:(i + 1) * chunk, :1]
                total = total + jnp.where(column == before, carried, 0.0)
            power = jnp.mean(total * total, axis=-1, keepdims=True)
            hidden[now, value_cols] = (total * lax.rsqrt(power + 1.0)).astype(jnp.bfloat16)

    lax.fori_loop(0, heads, head, 0)

    def close_step(h, _):
        if peers > 1:
            pl.when(s > 0)(lambda: close(h, True))
            pl.when(s == 0)(lambda: close(h, False))
        else:
            close(h, False)
        relays_at(h, CLOSING if planned else [])
        return 0

    lax.fori_loop(0, heads, close_step, 0)

    def plane_start(g):
        return pl.multiple_of(plane_at(g) * plane_rows, plane_rows)

    def add(g, cols, first, final):
        start = plane_start(g)
        product = mm(hidden[:, pl.ds(start, plane_rows)], w_ref[pl.ds(start, plane_rows), cols])
        if not first:
            product = acc[:, cols] + product
        if final:
            out_ref[:, cols] = product.astype(jnp.bfloat16)
        else:
            acc[:, cols] = product

    def project(g):
        for tile in range(columns // TILE):
            add(g, pl.ds(tile * TILE, TILE), False, False)

    def settle(g, piece, final=False):
        mirrored(g, piece)
        for core in range(peers):
            cols = pl.ds(pl.multiple_of(core * part + piece * width, width), width)
            add(g, cols, isinstance(g, int) and g == 0, final)

    def loop(lo, hi, body):
        def one(index, _):
            body(index)
            return 0

        lax.fori_loop(lo, hi, one, 0)

    def later(d):
        stage_all(d)
        front_all(d)

    def middle(g):
        finish(g, beside=False, ahead=False)
        loop(0, pieces, lambda piece: mirrored(g, piece))
        project(g)

    def opening(piece):
        stage(3, piece)
        settle(0, piece)

    def tidy(piece):
        finish(Z - 2, piece, piece + 1, beside=False)
        if Z > 3:
            finish(Z - 3, piece, piece + 1, beside=False, ahead=False)

    def streaming(piece):
        stage(Z, piece)

        @pl.when(piece > 0)
        def _():
            tidy(piece - 1)

        @pl.when(piece > 1)
        def _():
            stream(piece - 2)

    def stream(piece):
        for g in range(max(Z - 3, 1), Z - 1):
            settle(g, piece)

    def closing(piece):
        stage(Z + 1, piece)
        finish(Z - 1, piece, piece + 1)

        @pl.when(piece > 0)
        def _():
            settle(Z - 1, piece - 1, final=True)

    relay_steps(CLOSING[-1][1][1] if planned else 0, 2 * pieces)
    front_all(2)
    finish(0)
    if Z > 3:
        loop(0, pieces, opening)
        front_all(3)
        loop(4, Z, later)
    elif Z > 1:
        loop(0, pieces, lambda piece: settle(0, piece))
    if Z > 2:
        loop(1, Z - 2, lambda g: finish(g, rest=False))
        finish(Z - 2, rest=False, ahead=False)
        loop(1, Z - 3, middle)
        loop(0, pieces, streaming)
        tidy(pieces - 1)
        loop(max(pieces - 2, 0), pieces, stream)
    if Z > 1:
        loop(0, pieces, closing)

    @pl.when(s < peers - 1)
    def _():
        seg_copy.wait_send()

        def sent(h, _):
            state_copy(h).wait_send()
            return 0

        lax.fori_loop(0, heads, sent, 0)

    if sides:
        bulk(Z * len(sides), side_sem.at[0], recv_sem.at[0]).wait_send()
    if fronts:
        bulk(Z * len(fronts), side_sem.at[1], recv_sem.at[0]).wait_send()

    def sent_plane(plane, _):
        if corners:
            @pl.when(jnp.abs(plane - a) <= reach)
            def _():
                bulk(len(corners), relay_sem.at[plane], recv_sem.at[0]).wait_send()

        for side in (-1, 1):
            away = (a - plane) * side
            on = jnp.logical_and(has[side], away >= 0)

            @pl.when(on)
            def _():
                bulk(1, climb_sem.at[(side + 1) // 2, plane], recv_sem.at[0]).wait_send()

            if corners:
                @pl.when(jnp.logical_and(on, away + 1 > reach_by[side]))
                def _():
                    bulk(len(corners), corner_sem.at[(side + 1) // 2, plane], recv_sem.at[0]).wait_send()

        return 0

    lax.fori_loop(0, Z, sent_plane, 0)
    if Z > 1:
        settle(Z - 1, pieces - 1, final=True)
    else:
        loop(0, pieces, lambda piece: settle(0, piece, final=True))
    if X * Y * Z > 1:
        for ds in range(1, peers):
            bulk(X * Y * Z - 1, msend.at[ds - 1], recv_sem.at[0]).wait_send()


def local(grid, peers, queries, keys, values, gate_rate, segment_ids, decay_exps, out_weight):
    groups, length, key_features = queries.shape
    heads = decay_exps.shape[0]
    features = values.shape[2]
    columns = out_weight.shape[1]
    chips = grid[0] * grid[1] * grid[2]
    chunk = min(CHUNK, length)
    kw, vw = key_features // heads, features // heads
    bf16, f32 = jnp.bfloat16, jnp.float32
    anywhere = pl.BlockSpec(memory_space=pl.ANY)
    call = pl.pallas_call(
        functools.partial(kernel, grid, peers, heads, chunk, PIECES),
        out_shape=pltpu.VMEM((length, columns), bf16),
        in_specs=[anywhere] * 4
        + [pl.BlockSpec(memory_space=pltpu.VMEM), pl.BlockSpec(memory_space=pltpu.SMEM), anywhere],
        out_specs=pl.BlockSpec(memory_space=pltpu.VMEM),
        scratch_shapes=[
            pltpu.VMEM((length, key_features), bf16),
            pltpu.VMEM((length, key_features), bf16),
            pltpu.VMEM((length, features), bf16),
            pltpu.VMEM((length, key_features), bf16),
            pltpu.VMEM((features, columns), bf16),
            pltpu.VMEM((length, features), bf16),
            pltpu.VMEM((length, columns), f32),
            pltpu.VMEM((length, features), f32),
            pltpu.VMEM((1, length), jnp.int32),
            pltpu.VMEM((heads, vw, kw), f32),
            pltpu.VMEM((heads, vw, kw), f32),
            pltpu.SemaphoreType.DMA((5,)),
            pltpu.SemaphoreType.DMA((2,)),
            pltpu.SemaphoreType.DMA((heads,)),
            pltpu.SemaphoreType.DMA((heads,)),
            pltpu.SemaphoreType.DMA((2,)),
            pltpu.SemaphoreType.DMA((grid[0],)),
            pltpu.SemaphoreType.DMA((2, grid[0])),
            pltpu.SemaphoreType.DMA((2, grid[0])),
            pltpu.SemaphoreType.DMA((chips * PIECES,)),
            pltpu.SemaphoreType.DMA((max(peers - 1, 1),)),
            pltpu.SemaphoreType.DMA((max(peers - 1, 1), grid[0] * PIECES)),
        ],
        compiler_params=pltpu.CompilerParams(
            collective_id=0, has_side_effects=True, vmem_limit_bytes=61 * 1024 * 1024
        ),
        name="gla_project",
    )
    outs = [
        call(queries[n], keys[n], values[n], gate_rate[n], segment_ids[n:n + 1], decay_exps, out_weight)
        for n in range(groups)
    ]
    return jnp.stack(outs)


def solution(mesh):
    in_specs = (
        P("batch", "seq", None),
        P("batch", "seq", None),
        P("batch", "seq", None),
        P("batch", "seq", None),
        P("batch", "seq"),
        P(),
        P("batch", None),
    )
    body = functools.partial(local, chip_grid(mesh), mesh.shape["seq"])
    return jax.shard_map(
        body, mesh=mesh, in_specs=in_specs, out_specs=P("batch", "seq", None), check_vma=False
    )
```

```python
import functools
import math

import jax
import jax.numpy as jnp
from jax import lax
from jax.experimental import pallas as pl
from jax.experimental.pallas import tpu as pltpu
from jax.sharding import PartitionSpec as P

MESH = pl.DeviceIdType.MESH
CHUNK = 256
TILE = 512
PIECES = 4
OPENING = [(1, (0, 1)), (2, (1, 4)), (3, (4, 6))]
CLOSING = [(0, (6, 7)), (1, (7, 8))]


def chip_grid(mesh):
    count = mesh.shape["batch"]
    try:
        axis = mesh.axis_names.index("batch")
        line = mesh.devices.swapaxes(0, axis).reshape(count, -1)[:, 0]
        coords = [tuple(device.coords) for device in line]
        sizes = [len({c[i] for c in coords}) for i in (2, 1, 0)]
        lows = [min(c[i] for c in coords) for i in (2, 1, 0)]
        for index, c in enumerate(coords):
            z, y, x = (c[2] - lows[0], c[1] - lows[1], c[0] - lows[2])
            if (z * sizes[1] + y) * sizes[2] + x != index:
                return (count, 1, 1)
        return tuple(sizes)
    except Exception:
        return (count, 1, 1)


def split(x):
    high = x.astype(jnp.bfloat16)
    return high, (x - high.astype(jnp.float32)).astype(jnp.bfloat16)


def mm(a, b):
    return lax.dot_general(a, b, (((1,), (0,)), ((), ())), preferred_element_type=jnp.float32)


def mm_t(a, b):
    return lax.dot_general(a, b, (((1,), (1,)), ((), ())), preferred_element_type=jnp.float32)


def t_mm(a, b):
    return lax.dot_general(a, b, (((0,), (0,)), ((), ())), preferred_element_type=jnp.float32)


def thresholds(grid):
    Z, Y, X = grid
    beside, corner = X + Y - 2, (X - 1) * (Y - 1)
    picked = []
    for a in range(Z):
        best = None
        for reach in range(Z):
            far = [g for g in range(Z) if abs(g - a) > reach]
            below = a + corner * len([g for g in far if g < a])
            above = Z - 1 - a + corner * len([g for g in far if g > a])
            inside = (Z * beside + (Z - len(far)) * corner) / 2
            load = max(below, above, inside)
            if best is None or load < best[0]:
                best = (load, reach)
        picked.append(best[1])
    return picked


def kernel(
    grid, peers, heads, chunk, pieces,
    q_hbm, k_hbm, v_hbm, g_hbm, seg_ref, exps_ref, w_hbm,
    out_ref,
    q_ref, k_ref, v_ref, g_ref, w_ref, hidden, acc, mixed, seg_in, state_in, state_out,
    load_sem, seg_sem, state_send, state_recv, side_sem, relay_sem, climb_sem, corner_sem, recv_sem, msend, mrecv, mwhole,
):
    Z, Y, X = grid
    s = lax.axis_index("seq")
    me = lax.axis_index("batch")
    length, keys = q_ref.shape
    key_width = keys // heads
    value_width = v_ref.shape[1] // heads
    rows = w_hbm.shape[0]
    columns = w_ref.shape[1]
    part = columns // peers
    width = part // pieces
    plane_rows = rows * X * Y
    a = me // (X * Y)
    swap = X == Y
    nb, nc = X, Y
    sides = [(db, 0) for db in range(1, nb)]
    fronts = [(0, dc) for dc in range(1, nc)]
    corners = [(db, dc) for db in range(1, nb) for dc in range(1, nc)]
    table = thresholds(grid)

    def strides(core):
        if not swap:
            return 1, X
        even = lax.rem(core, 2) == 0
        return jnp.where(even, 1, X), jnp.where(even, X, 1)

    def chip_at(core, plane, db, dc):
        sb, sc = strides(core)
        b = lax.rem(me // sb, nb)
        c = lax.rem(me // sc, nc)
        return (
            plane * (X * Y)
            + lax.rem(b - db + nb, nb) * sb
            + lax.rem(c - dc + nc, nc) * sc
        )

    near = jnp.minimum(a, Z - 1 - a)

    def plane_at(g):
        side = jnp.where(lax.rem(g, 2) == 1, -1, 1)
        rest = jnp.where(a < Z - 1 - a, g, Z - 1 - g)
        return jnp.where(g <= 2 * near, a + (g + 1) // 2 * side, rest)

    def reach_of(plane):
        reach = jnp.int32(table[0])
        for index in range(1, Z):
            reach = jnp.where(plane == index, table[index], reach)
        return reach

    reach = reach_of(a)
    reach_by = {-1: reach_of(a - 1), 1: reach_of(a + 1)}
    has = {-1: a > 0, 1: a < Z - 1}

    def label(plane, db, dc):
        return (plane * nb + db) * nc + dc

    def block(core, start, count, piece, pieces_wide=1):
        return w_ref.at[
            pl.ds(pl.multiple_of(start, rows), count),
            pl.ds(pl.multiple_of(core * part + piece * width, width), pieces_wide * width),
        ]

    def send(held, to, sem, device, piece):
        here = block(s, chip_at(s, *held) * rows, rows, piece)
        return pltpu.make_async_remote_copy(
            src_ref=here, dst_ref=here, send_sem=sem, recv_sem=recv_sem.at[label(*to) * pieces + piece],
            device_id={"batch": device}, device_id_type=MESH,
        )

    def sideways(plane, piece):
        for db, _ in sides:
            send((plane, 0, 0), (plane, db, 0), side_sem.at[0], chip_at(s, a, -db, 0), piece).start()

    def forwards(plane, piece):
        for _, dc in fronts:
            send((plane, 0, 0), (plane, 0, dc), side_sem.at[1], chip_at(s, a, 0, -dc), piece).start()

    def climb(plane, side, piece):
        to = (plane, 0, 0)
        send(to, to, climb_sem.at[(side + 1) // 2, plane], me + side * X * Y, piece).start()

    def climb_corners(plane, side, piece):
        for corner in corners:
            to = (plane, *corner)
            send(to, to, corner_sem.at[(side + 1) // 2, plane], me + side * X * Y, piece).start()

    def wait_piece(plane, db, dc, piece):
        to = (plane, db, dc)
        send(to, to, side_sem.at[0], lax.rem(me + 1, X * Y * Z), piece).wait_recv()

    def share(plane, db, dc, piece):
        here = block(s, chip_at(s, plane, db, dc) * rows, rows, piece)
        for ds in range(1, peers):
            pltpu.make_async_remote_copy(
                src_ref=here, dst_ref=here,
                send_sem=msend.at[ds - 1], recv_sem=mrecv.at[ds - 1, plane * pieces + piece],
                device_id={"seq": lax.rem(s + ds, peers)}, device_id_type=MESH,
            ).start()

    def share_whole(plane, db, dc, piece):
        @pl.when(piece == pieces - 1)
        def _():
            here = block(s, chip_at(s, plane, db, dc) * rows, rows, 0, pieces)
            for ds in range(1, peers):
                pltpu.make_async_remote_copy(
                    src_ref=here, dst_ref=here, send_sem=msend.at[ds - 1], recv_sem=mwhole.at[ds - 1, plane],
                    device_id={"seq": lax.rem(s + ds, peers)}, device_id_type=MESH,
                ).start()

    def bulk(count, send_end, recv_end, core=0, piece=0, pieces_wide=pieces):
        here = block(core, 0, count * rows, piece, pieces_wide)
        return pltpu.make_async_remote_copy(
            src_ref=here, dst_ref=here, send_sem=send_end, recv_sem=recv_end,
            device_id={"batch": lax.rem(me + 1, X * Y * Z)}, device_id_type=MESH,
        )

    def inside(plane):
        return jnp.logical_and(plane >= 0, plane < Z)

    def needs(distance, side):
        return jnp.logical_and(has[side], distance + 1 > reach_by[side])

    def stage(d, piece):
        for side in (-1, 1):
            plane = a + side * d

            @pl.when(inside(plane))
            def _():
                wait_piece(plane, 0, 0, piece)
                pl.when(has[-side])(lambda: climb(plane, -side, piece))
                pl.when(d < Z - 1)(lambda: sideways(plane, piece))
                share_whole(plane, 0, 0, piece)

        @pl.when(d == 1)
        def _():
            for db, _ in sides:
                wait_piece(a, db, 0, piece)
                for _, dc in fronts:
                    send((a, db, 0), (a, db, dc), relay_sem.at[a], chip_at(s, a, 0, -dc), piece).start()
                share_whole(a, db, 0, piece)

        if not corners:
            return

        f = d - 2
        for side in (-1, 1):
            plane = a + side * f

            @pl.when(jnp.logical_and(jnp.logical_and(f > 0, f <= reach), inside(plane)))
            def _():
                for _, dc in fronts:
                    wait_piece(plane, 0, dc, piece)
                    for db, _ in sides:
                        send(
                            (plane, 0, dc), (plane, db, dc), relay_sem.at[plane],
                            chip_at(s, a, -db, 0), piece,
                        ).start()
                    share(plane, 0, dc, piece)

        def corner_step(plane, distance, side, both):
            for corner in corners:
                wait_piece(plane, *corner, piece)
            pl.when(needs(distance, -side))(lambda: climb_corners(plane, -side, piece))
            if both:
                pl.when(needs(distance, side))(lambda: climb_corners(plane, side, piece))
            for corner in corners:
                (share_whole if both else share)(plane, *corner, piece)

        pl.when(d == 2)(lambda: corner_step(a, 0, -1, True))
        for side in (-1, 1):
            late = a + side * (d - 3)
            on = jnp.logical_and(jnp.logical_and(d > 3, d - 3 <= reach), needs(d - 3, -side))
            pl.when(jnp.logical_and(on, inside(late)))(lambda: corner_step(late, d - 3, side, False))
        for side in (-1, 1):
            far = a + side * f
            on = jnp.logical_and(jnp.logical_and(f > 0, f > reach), inside(far))
            pl.when(on)(lambda: corner_step(far, f, side, False))

    def stage_all(d, lo=0, hi=pieces):
        def one(piece, _):
            stage(d, piece)
            return 0

        lax.fori_loop(lo, hi, one, 0)

    def front_all(d):
        def one(piece, _):
            for side in (-1, 1):
                plane = a + side * d

                @pl.when(inside(plane))
                def _():
                    pl.when(d == Z - 1)(lambda: sideways(plane, piece))
                    forwards(plane, piece)
            return 0

        lax.fori_loop(0, pieces, one, 0)

    def finish(g, lo=0, hi=pieces, beside=True, rest=True, ahead=True):
        plane = plane_at(g)
        distance = jnp.abs(plane - a)
        side = jnp.where(plane < a, -1, 1)
        onward = jnp.where(side < 0, needs(distance, 1), needs(distance, -1))
        near_by = distance <= reach

        def one(piece, _):
            if beside:
                for db, _ in sides:
                    @pl.when(distance > 0)
                    def _():
                        wait_piece(plane, db, 0, piece)
                        share(plane, db, 0, piece)

            if ahead:
                for _, dc in fronts:
                    @pl.when(jnp.logical_or(distance == 0, jnp.logical_not(near_by)) if corners else distance >= 0)
                    def _():
                        wait_piece(plane, 0, dc, piece)
                        (share_whole if isinstance(g, int) and g == 0 else share)(plane, 0, dc, piece)

            if corners and rest:
                late = jnp.logical_and(near_by, jnp.logical_not(onward))

                @pl.when(jnp.logical_and(late, distance > 0))
                def _():
                    for corner in corners:
                        wait_piece(plane, *corner, piece)
                        share(plane, *corner, piece)
            return 0

        lax.fori_loop(lo, hi, one, 0)

    def mirrored(g, piece):
        plane = plane_at(g)
        own_plane = isinstance(g, int) and g == 0
        for ds in range(1, peers):
            core = lax.rem(s - ds + peers, peers)
            count = X * Y - 1

            @pl.when(piece == 0)
            def _():
                bulk(count if own_plane else 1, msend.at[ds - 1], mwhole.at[ds - 1, plane], core).wait_recv()

            if count and not own_plane:
                bulk(
                    count, msend.at[ds - 1], mrecv.at[ds - 1, plane * pieces + piece], core, piece, 1
                ).wait_recv()

    loads = [
        pltpu.make_async_copy(
            w_hbm, w_ref.at[pl.ds(pl.multiple_of(me * rows, rows), rows), :], load_sem.at[0]
        ),
        pltpu.make_async_copy(g_hbm, g_ref, load_sem.at[1]),
        pltpu.make_async_copy(k_hbm, k_ref, load_sem.at[2]),
        pltpu.make_async_copy(q_hbm, q_ref, load_sem.at[3]),
        pltpu.make_async_copy(v_hbm, v_ref, load_sem.at[4]),
    ]
    for load in loads:
        load.start()

    barrier = pltpu.get_barrier_semaphore()
    friends = [{"batch": chip_at(s, a, d, 0)} for d in range(1, nb)]
    friends += [{"batch": chip_at(s, a, 0, d)} for d in range(1, nc)]
    friends += [{"seq": lax.rem(s + d, peers)} for d in range(1, peers)]
    for friend in friends:
        pl.semaphore_signal(barrier, inc=1, device_id=friend, device_id_type=MESH)

    @pl.when(a < Z - 1)
    def _():
        pl.semaphore_signal(barrier, inc=1, device_id={"batch": me + X * Y}, device_id_type=MESH)

    @pl.when(a > 0)
    def _():
        pl.semaphore_signal(barrier, inc=1, device_id={"batch": me - X * Y}, device_id_type=MESH)

    above, below = jnp.where(a < Z - 1, 1, 0), jnp.where(a > 0, 1, 0)
    pl.semaphore_wait(barrier, len(friends) + above + below)

    loads[0].wait()

    def own(piece, _):
        for side in (-1, 1):
            pl.when(has[side])(lambda: climb(a, side, piece))
        sideways(a, piece)
        forwards(a, piece)
        return 0

    lax.fori_loop(0, pieces, own, 0)

    def next_core():
        return {"seq": lax.rem(s + 1, peers)}

    seg_copy = pltpu.make_async_remote_copy(
        src_ref=seg_ref, dst_ref=seg_in, send_sem=seg_sem.at[0], recv_sem=seg_sem.at[1],
        device_id=next_core(), device_id_type=MESH,
    )

    def state_copy(h):
        return pltpu.make_async_remote_copy(
            src_ref=state_out.at[h], dst_ref=state_in.at[h],
            send_sem=state_send.at[h], recv_sem=state_recv.at[h],
            device_id=next_core(), device_id_type=MESH,
        )

    @pl.when(s < peers - 1)
    def _():
        seg_copy.start()

    @pl.when(s == 0)
    def _():
        seg_in[...] = jnp.full(seg_in.shape, -1, jnp.int32)

    for load in loads[1:]:
        load.wait()

    @pl.when(s > 0)
    def _():
        seg_copy.wait_recv()

    order_t = lax.broadcasted_iota(jnp.int32, (chunk, chunk), 0)
    order_s = lax.broadcasted_iota(jnp.int32, (chunk, chunk), 1)
    causal = order_t >= order_s
    triangle = jnp.where(causal, 1.0, 0.0).astype(jnp.bfloat16)
    seg_row = seg_ref[...].astype(jnp.float32)
    before = seg_in[...].astype(jnp.float32)[:, length - 1:]
    seg_wide = jnp.broadcast_to(seg_row, (128, length)).T

    def relay_steps(lo, hi):
        def one(number, _):
            stage(1 + number // pieces, lax.rem(number, pieces))
            pl.when(number == pieces - 1)(lambda: front_all(1))
            return 0

        lax.fori_loop(lo, hi, one, 0)

    def relays_at(h, plan):
        lo = hi = 0
        for at, (start, stop) in plan:
            lo, hi = jnp.where(h == at, start, lo), jnp.where(h == at, stop, hi)
        relay_steps(lo, hi)

    planned = heads == 4 and pieces == 4

    def columns_of(h):
        key_cols = pl.ds(pl.multiple_of(h * key_width, key_width), key_width)
        return key_cols, pl.ds(pl.multiple_of(h * value_width, value_width), value_width)

    def head(h, _):
        relays_at(h, OPENING if planned else [])

        exponent = jnp.full((1, key_width), exps_ref[h], jnp.int32).astype(jnp.float32)
        scale = jnp.exp2(-exponent) * (-1.0 / 16.0)
        key_cols, value_cols = columns_of(h)
        state = previous = offset = None
        for i in range(length // chunk):
            now = pl.ds(i * chunk, chunk)
            log = mm(triangle, g_ref[now, key_cols]) * scale
            fall = jnp.exp(log)
            raised_q = q_ref[now, key_cols].astype(jnp.float32) * (fall * (1.0 / math.sqrt(key_width)))
            raised_k = k_ref[now, key_cols].astype(jnp.float32) * jnp.exp(-log)
            value = v_ref[now, value_cols]
            q_hi, q_lo = split(raised_q)
            k_hi, k_lo = split(raised_k)
            row = seg_row[:, i * chunk:(i + 1) * chunk]
            column = seg_wide[i * chunk:(i + 1) * chunk, :1]
            scores = mm_t(q_hi, k_hi) + mm_t(q_hi, k_lo) + mm_t(q_lo, k_hi)
            scores = jnp.where(jnp.logical_and(causal, column == row), scores, 0.0)
            p_hi, p_lo = split(scores)
            inner = mm(p_hi, value) + mm(p_lo, value)
            if i > 0:
                s_hi, s_lo = split(state)
                carried = mm_t(q_hi, s_hi) + mm_t(q_hi, s_lo) + mm_t(q_lo, s_hi)
                inner = inner + jnp.where(column == previous, carried, 0.0)
            mixed[now, value_cols] = inner
            if peers > 1:
                whole = raised_q if i == 0 else raised_q * jnp.exp(offset)
                q_ref[now, key_cols], g_ref[now, key_cols] = split(whole)
            final = fall[chunk - 1:, :]
            end = log[chunk - 1:, :]
            offset = end if i == 0 else offset + end
            last = row[:, chunk - 1:]
            weighted = jnp.where(column == last, raised_k * final, 0.0)
            w_hi, w_lo = split(weighted)
            grown = t_mm(value, w_hi) + t_mm(value, w_lo)
            state = grown if i == 0 else grown + jnp.where(last == previous, state * final, 0.0)
            previous = last

        if peers > 1:
            @pl.when(s == 0)
            def _():
                state_out[h] = state
                state_copy(h).start()

        if peers > 2:
            @pl.when(jnp.logical_and(s > 0, s < peers - 1))
            def _():
                state_copy(h).wait_recv()
                state_out[h] = state + jnp.where(previous == before, state_in[h] * jnp.exp(offset), 0.0)
                state_copy(h).start()

        return 0

    def close(h, carry):
        key_cols, value_cols = columns_of(h)
        if carry:
            if peers > 2:
                pl.when(s == peers - 1)(lambda: state_copy(h).wait_recv())
            else:
                state_copy(h).wait_recv()
            s_hi, s_lo = split(state_in[h])
        for i in range(length // chunk):
            now = pl.ds(i * chunk, chunk)
            total = mixed[now, value_cols]
            if carry:
                q_hi, q_lo = q_ref[now, key_cols], g_ref[now, key_cols]
                carried = mm_t(q_hi, s_hi) + mm_t(q_hi, s_lo) + mm_t(q_lo, s_hi)
                column = seg_wide[i * chunk:(i + 1) * chunk, :1]
                total = total + jnp.where(column == before, carried, 0.0)
            power = jnp.mean(total * total, axis=-1, keepdims=True)
            hidden[now, value_cols] = (total * lax.rsqrt(power + 1.0)).astype(jnp.bfloat16)

    lax.fori_loop(0, heads, head, 0)

    def close_step(h, _):
        if peers > 1:
            pl.when(s > 0)(lambda: close(h, True))
            pl.when(s == 0)(lambda: close(h, False))
        else:
            close(h, False)
        relays_at(h, CLOSING if planned else [])
        return 0

    lax.fori_loop(0, heads, close_step, 0)

    def plane_start(g):
        return pl.multiple_of(plane_at(g) * plane_rows, plane_rows)

    def add(g, cols, first, final):
        start = plane_start(g)
        product = mm(hidden[:, pl.ds(start, plane_rows)], w_ref[pl.ds(start, plane_rows), cols])
        if not first:
            product = acc[:, cols] + product
        if final:
            out_ref[:, cols] = product.astype(jnp.bfloat16)
        else:
            acc[:, cols] = product

    def project(g):
        for tile in range(columns // TILE):
            add(g, pl.ds(tile * TILE, TILE), False, False)

    def settle(g, piece, final=False):
        mirrored(g, piece)
        for core in range(peers):
            cols = pl.ds(pl.multiple_of(core * part + piece * width, width), width)
            add(g, cols, isinstance(g, int) and g == 0, final)

    def loop(lo, hi, body):
        def one(index, _):
            body(index)
            return 0

        lax.fori_loop(lo, hi, one, 0)

    def later(d):
        stage_all(d)
        front_all(d)

    def middle(g):
        finish(g, beside=False, ahead=False)
        loop(0, pieces, lambda piece: mirrored(g, piece))
        project(g)

    def opening(piece):
        stage(3, piece)
        settle(0, piece)

    def tidy(piece):
        finish(Z - 2, piece, piece + 1, beside=False)
        if Z > 3:
            finish(Z - 3, piece, piece + 1, beside=False, ahead=False)

    def streaming(piece):
        stage(Z, piece)

        @pl.when(piece > 0)
        def _():
            tidy(piece - 1)

        @pl.when(piece > 1)
        def _():
            stream(piece - 2)

    def stream(piece):
        for g in range(max(Z - 3, 1), Z - 1):
            settle(g, piece)

    def closing(piece):
        stage(Z + 1, piece)
        finish(Z - 1, piece, piece + 1)

        @pl.when(piece > 0)
        def _():
            settle(Z - 1, piece - 1, final=True)

    relay_steps(CLOSING[-1][1][1] if planned else 0, 2 * pieces)
    front_all(2)
    finish(0)
    if Z > 3:
        loop(0, pieces, opening)
        front_all(3)
        loop(4, Z, later)
    elif Z > 1:
        loop(0, pieces, lambda piece: settle(0, piece))
    if Z > 2:
        loop(1, Z - 2, lambda g: finish(g, rest=False))
        finish(Z - 2, rest=False, ahead=False)
        loop(1, Z - 3, middle)
        loop(0, pieces, streaming)
        tidy(pieces - 1)
        loop(max(pieces - 2, 0), pieces, stream)
    if Z > 1:
        loop(0, pieces, closing)

    @pl.when(s < peers - 1)
    def _():
        seg_copy.wait_send()

        def sent(h, _):
            state_copy(h).wait_send()
            return 0

        lax.fori_loop(0, heads, sent, 0)

    if sides:
        bulk(Z * len(sides), side_sem.at[0], recv_sem.at[0]).wait_send()
    if fronts:
        bulk(Z * len(fronts), side_sem.at[1], recv_sem.at[0]).wait_send()

    def sent_plane(plane, _):
        if corners:
            @pl.when(jnp.abs(plane - a) <= reach)
            def _():
                bulk(len(corners), relay_sem.at[plane], recv_sem.at[0]).wait_send()

        for side in (-1, 1):
            away = (a - plane) * side
            on = jnp.logical_and(has[side], away >= 0)

            @pl.when(on)
            def _():
                bulk(1, climb_sem.at[(side + 1) // 2, plane], recv_sem.at[0]).wait_send()

            if corners:
                @pl.when(jnp.logical_and(on, away + 1 > reach_by[side]))
                def _():
                    bulk(len(corners), corner_sem.at[(side + 1) // 2, plane], recv_sem.at[0]).wait_send()

        return 0

    lax.fori_loop(0, Z, sent_plane, 0)
    if Z > 1:
        settle(Z - 1, pieces - 1, final=True)
    else:
        loop(0, pieces, lambda piece: settle(0, piece, final=True))
    if X * Y * Z > 1:
        for ds in range(1, peers):
            bulk(X * Y * Z - 1, msend.at[ds - 1], recv_sem.at[0]).wait_send()


def local(grid, peers, queries, keys, values, gate_rate, segment_ids, decay_exps, out_weight):
    groups, length, key_features = queries.shape
    heads = decay_exps.shape[0]
    features = values.shape[2]
    columns = out_weight.shape[1]
    chips = grid[0] * grid[1] * grid[2]
    chunk = min(CHUNK, length)
    kw, vw = key_features // heads, features // heads
    bf16, f32 = jnp.bfloat16, jnp.float32
    anywhere = pl.BlockSpec(memory_space=pl.ANY)
    call = pl.pallas_call(
        functools.partial(kernel, grid, peers, heads, chunk, PIECES),
        out_shape=pltpu.VMEM((length, columns), bf16),
        in_specs=[anywhere] * 4
        + [pl.BlockSpec(memory_space=pltpu.VMEM), pl.BlockSpec(memory_space=pltpu.SMEM), anywhere],
        out_specs=pl.BlockSpec(memory_space=pltpu.VMEM),
        scratch_shapes=[
            pltpu.VMEM((length, key_features), bf16),
            pltpu.VMEM((length, key_features), bf16),
            pltpu.VMEM((length, features), bf16),
            pltpu.VMEM((length, key_features), bf16),
            pltpu.VMEM((features, columns), bf16),
            pltpu.VMEM((length, features), bf16),
            pltpu.VMEM((length, columns), f32),
            pltpu.VMEM((length, features), f32),
            pltpu.VMEM((1, length), jnp.int32),
            pltpu.VMEM((heads, vw, kw), f32),
            pltpu.VMEM((heads, vw, kw), f32),
            pltpu.SemaphoreType.DMA((5,)),
            pltpu.SemaphoreType.DMA((2,)),
            pltpu.SemaphoreType.DMA((heads,)),
            pltpu.SemaphoreType.DMA((heads,)),
            pltpu.SemaphoreType.DMA((2,)),
            pltpu.SemaphoreType.DMA((grid[0],)),
            pltpu.SemaphoreType.DMA((2, grid[0])),
            pltpu.SemaphoreType.DMA((2, grid[0])),
            pltpu.SemaphoreType.DMA((chips * PIECES,)),
            pltpu.SemaphoreType.DMA((max(peers - 1, 1),)),
            pltpu.SemaphoreType.DMA((max(peers - 1, 1), grid[0] * PIECES)),
            pltpu.SemaphoreType.DMA((max(peers - 1, 1), grid[0])),
        ],
        compiler_params=pltpu.CompilerParams(
            collective_id=0, has_side_effects=True, vmem_limit_bytes=61 * 1024 * 1024
        ),
        name="gla_project",
    )
    outs = [
        call(queries[n], keys[n], values[n], gate_rate[n], segment_ids[n:n + 1], decay_exps, out_weight)
        for n in range(groups)
    ]
    return jnp.stack(outs)


def solution(mesh):
    in_specs = (
        P("batch", "seq", None),
        P("batch", "seq", None),
        P("batch", "seq", None),
        P("batch", "seq", None),
        P("batch", "seq"),
        P(),
        P("batch", None),
    )
    body = functools.partial(local, chip_grid(mesh), mesh.shape["seq"])
    return jax.shard_map(
        body, mesh=mesh, in_specs=in_specs, out_specs=P("batch", "seq", None), check_vma=False
    )
```
